32 devices in a mesh: sys: 1 (over z), aux: 4 (over y), orb: 8 (over x, core).
Axes of the slice: x: 4, y: 4, z: 1, core: 2. Of those that a mesh axis runs over, the one named last changes fastest.
The devices are a block of a 4x4x8 slice.
Arguments:
- aux_ints: float32 [1344, 384, 384], P(('sys', 'aux'), 'orb')
- metric: float32 [1344, 1344], P(('sys', 'aux'))
- orbitals: float32 [4, 384, 80], P('sys')
Outputs:
- output: float32 [4, 384, 384], P('sys', 'orb', 'aux')
All inputs are finite; a program needn't handle non-finite values.
Results may differ from the reference program's by a relative error of at most 0.001.
Values are sent between devices in bfloat16 or wider.
A program may use at most 768 MiB of HBM per device.

```python
import jax
import jax.numpy as jnp
from jax import lax

N_AUX = 1344
N_BASIS = 384
N_OCC = 80
DENS = 4

PRECISE = lax.Precision.HIGHEST


def setup_inputs(seed: int = 0, part: int = 0) -> dict:
    base_key = jax.random.fold_in(jax.random.key(seed), part)
    sub_keys = jax.random.split(base_key, 6)
    rank_b = 4
    rank_m = 4
    coh_scale = (2.0 * N_AUX * N_OCC) ** -0.5 * rank_b ** -0.25
    noise_scale = 2.0 * coh_scale
    coeffs = jax.random.normal(sub_keys[0], (N_AUX, rank_b), jnp.float32)
    patterns = jax.random.normal(sub_keys[1], (rank_b, N_BASIS), jnp.float32)
    row_keys = jax.random.split(sub_keys[2], N_AUX)

    def one_row(row_args):
        row_key, coeff_row = row_args
        noise_mat = jax.random.normal(row_key, (N_BASIS, N_BASIS), jnp.float32)
        sym_noise = (noise_mat + noise_mat.T) * (0.5 ** 0.5)
        low_rank = jnp.einsum('k,km,kl->ml', coeff_row, patterns, patterns)
        return noise_scale * sym_noise + coh_scale * low_rank

    aux_ints = lax.map(one_row, (row_keys, coeffs))
    spread = jax.random.normal(sub_keys[3], (N_AUX, N_AUX), jnp.float32)
    sym_spread = (spread + spread.T) * (0.125 / N_AUX) ** 0.5
    directions = jax.random.normal(sub_keys[4], (rank_m, N_AUX), jnp.float32) * N_AUX ** -0.5
    boost_scale = (N_AUX / rank_m) ** 0.5
    metric = jnp.eye(N_AUX, dtype=jnp.float32) + sym_spread + boost_scale * jnp.dot(directions.T, directions)
    orbitals = jax.random.normal(sub_keys[5], (DENS, N_BASIS, N_OCC), jnp.float32) * N_BASIS ** -0.5
    return {'aux_ints': aux_ints, 'metric': metric, 'orbitals': orbitals}


def reference(aux_ints, metric, orbitals):
    def one_density(coeff_mat):
        half_tr = jnp.einsum('qml,li->qmi', aux_ints, coeff_mat, precision=PRECISE)
        fitted = jnp.einsum('pq,qmi->pmi', metric, half_tr, precision=PRECISE)
        exchange = jnp.einsum('pmi,pni->mn', fitted, fitted, precision=PRECISE)
        gamma_raw = jnp.einsum('qmi,mi->q', half_tr, coeff_mat, precision=PRECISE)
        gamma_fit = jnp.dot(metric, gamma_raw, precision=PRECISE)
        weights = jnp.dot(gamma_fit, metric, precision=PRECISE)
        coulomb = jnp.einsum('q,qmn->mn', weights, aux_ints, precision=PRECISE)
        return 2.0 * coulomb - exchange

    return lax.map(one_density, orbitals)
```

```python
import jax
import jax.numpy as jnp
from jax import lax
from jax.experimental import pallas as pl
from jax.experimental.pallas import tpu as pltpu
from jax.sharding import PartitionSpec as P

PRECISE = lax.Precision.HIGHEST
F32 = jnp.float32
BF16 = jnp.bfloat16
MESH = pl.DeviceIdType.MESH


def exchange(x, axis, n, cid):
    def kernel(x_ref, o_ref, send_sem, recv_sem):
        me = lax.axis_index(axis)
        barrier = pltpu.get_barrier_semaphore()
        for r in range(1, n):
            pl.semaphore_signal(barrier, inc=1, device_id={axis: lax.rem(me + r, n)}, device_id_type=MESH)
        pl.semaphore_wait(barrier, n - 1)
        copies = []
        for r in range(1, n):
            to = lax.rem(me + r, n)
            copy = pltpu.make_async_remote_copy(
                src_ref=x_ref.at[to], dst_ref=o_ref.at[me], send_sem=send_sem.at[r], recv_sem=recv_sem.at[r],
                device_id={axis: to}, device_id_type=MESH)
            copy.start()
            copies.append(copy)
        for copy in copies:
            copy.wait()

    return pl.pallas_call(
        kernel,
        out_shape=jax.ShapeDtypeStruct(x.shape, x.dtype),
        in_specs=[pl.BlockSpec(memory_space=pl.ANY)],
        out_specs=pl.BlockSpec(memory_space=pl.ANY),
        scratch_shapes=[pltpu.SemaphoreType.DMA((n,)), pltpu.SemaphoreType.DMA((n,))],
        compiler_params=pltpu.CompilerParams(collective_id=cid, has_side_effects=True),
    )(x)


def solution(mesh):
    n_aux, n_orb = mesh.shape['aux'], mesh.shape['orb']

    def local_fock(ints, metric, orbitals):
        n_q, n_m, n_l = ints.shape
        n_d, _, n_i = orbitals.shape
        j, k = lax.axis_index('aux'), lax.axis_index('orb')
        half = jnp.einsum('qml,dli->dqmi', ints, orbitals, precision=PRECISE, preferred_element_type=F32)
        orb_rows = lax.dynamic_slice_in_dim(orbitals, k * n_m, n_m, axis=1)
        gamma = lax.psum(jnp.einsum('dqmi,dmi->dq', half, orb_rows, precision=PRECISE), 'orb')
        gamma = lax.all_gather(gamma, 'aux', axis=1, tiled=True)
        gamma_fit = jnp.einsum('dq,pq->dp', gamma, metric, precision=PRECISE)
        weights = lax.psum_scatter(jnp.dot(gamma_fit, metric, precision=PRECISE), 'aux', scatter_dimension=1, tiled=True)
        coul = jnp.einsum('dq,qmn->dmn', weights, ints, precision=PRECISE)
        coul = lax.psum_scatter(coul, 'aux', scatter_dimension=2, tiled=True)

        half = half.reshape(n_d, n_q, n_m * n_i)
        got = exchange(half.astype(BF16), 'aux', n_aux, 0)
        got = lax.dynamic_update_slice_in_dim(got, jnp.zeros((1,) + got.shape[1:], BF16), j, axis=0)
        own = lax.dynamic_index_in_dim(half, j, axis=0, keepdims=False)
        met = lax.all_gather(metric.astype(BF16), 'aux', axis=0, tiled=True)
        fit = jnp.einsum('qp,qx->px', metric, own, precision=PRECISE)
        fit = fit + jnp.einsum('qp,qx->px', met, got.reshape(n_aux * n_q, n_m * n_i), preferred_element_type=F32)
        n_p = fit.shape[0] // n_orb
        fit = fit.reshape(n_orb, n_p, n_m * n_i)
        all_t = exchange(fit.astype(BF16), 'orb', n_orb, 1)
        mine = lax.dynamic_index_in_dim(fit, k, axis=0, keepdims=True)
        mine_hi = lax.reduce_precision(mine, 8, 7)
        rest = mine - mine_hi
        all_t = lax.dynamic_update_slice_in_dim(all_t, mine_hi.astype(BF16), k, axis=0)
        all_t = all_t.reshape(n_orb, n_p, n_m, n_i)
        n_n = n_orb * n_m
        exch = jnp.einsum('kpmi,lpni->kmln', all_t, all_t, preferred_element_type=F32).reshape(n_n, n_n)
        side = lax.dynamic_update_slice_in_dim(
            all_t.astype(F32), (mine_hi + 0.5 * rest).reshape(1, n_p, n_m, n_i), k, axis=0)
        cross = jnp.einsum('pmi,lpni->mln', rest.reshape(n_p, n_m, n_i), side, precision=PRECISE).reshape(n_m, n_n)
        cross = lax.dynamic_update_slice_in_dim(jnp.zeros((n_n, n_n), F32), cross, k * n_m, axis=0)
        exch = exch + cross + cross.T
        exch = lax.psum_scatter(exch, 'orb', scatter_dimension=0, tiled=True)
        exch = lax.all_to_all(exch.reshape(n_m, n_aux, n_n // n_aux), 'aux', 1, 0)
        return 2.0 * coul - exch.reshape(n_d, n_m, n_n // n_aux)

    return jax.shard_map(local_fock, mesh=mesh, in_specs=(P(('sys', 'aux'), 'orb', None), P(('sys', 'aux'), None), P('sys', None, None)), out_specs=P('sys', 'orb', 'aux'), check_vma=False)
```

```python
import jax
import jax.numpy as jnp
from jax import lax
from jax.experimental import pallas as pl
from jax.experimental.pallas import tpu as pltpu
from jax.sharding import PartitionSpec as P

PRECISE = lax.Precision.HIGHEST
F32 = jnp.float32
BF16 = jnp.bfloat16
MESH = pl.DeviceIdType.MESH
LANES = 128
WIDE = 256
ROWS_M = 16


def round_up(n, to):
    return (n + to - 1) // to * to


def parts3(x):
    hi = x.astype(BF16)
    rest = x - hi.astype(F32)
    mid = rest.astype(BF16)
    return hi, mid, (rest - mid.astype(F32)).astype(BF16)


def fit_exchange(x, own, weights, n_aux, n_orb):
    n_c, _, n_rows, n_q = x.shape
    depth, n_p = weights.shape
    share = n_rows // n_orb
    half_rows = n_rows // 2

    def kernel(x_ref, own_ref, w_ref, t_ref, mine_ref, got, own_f, part, fit, out, y_send, y_recv, x_send, x_recv, loc, keep):
        j, k = lax.axis_index('aux'), lax.axis_index('orb')
        barrier = pltpu.get_barrier_semaphore()
        for r in range(1, n_aux):
            pl.semaphore_signal(barrier, inc=1, device_id={'aux': lax.rem(j + r, n_aux)}, device_id_type=MESH)
        for r in range(1, n_orb):
            pl.semaphore_signal(barrier, inc=1, device_id={'orb': lax.rem(k + r, n_orb)}, device_id_type=MESH)
        pl.semaphore_wait(barrier, n_aux + n_orb - 2)

        def y_copy(c, r):
            to = lax.rem(j + n_aux - r, n_aux)
            return pltpu.make_async_remote_copy(
                src_ref=x_ref.at[c, to], dst_ref=got.at[c, r - 1], send_sem=y_send.at[c, r - 1],
                recv_sem=y_recv.at[c, r - 1], device_id={'aux': to}, device_id_type=MESH)

        def x_copy(c, r):
            to = lax.rem(k + r, n_orb)
            return pltpu.make_async_remote_copy(
                src_ref=out.at[c, to], dst_ref=t_ref.at[k, c], send_sem=x_send.at[c, r - 1],
                recv_sem=x_recv.at[c, r - 1], device_id={'orb': to}, device_id_type=MESH)

        for c in range(n_c):
            for r in range(1, n_aux):
                y_copy(c, r).start()

        def own_copy(c):
            return pltpu.make_async_copy(own_ref.at[c], own_f, loc.at[0])

        def keep_copies(c):
            return (pltpu.make_async_copy(fit.at[k], mine_ref.at[c], keep.at[0]),
                    pltpu.make_async_copy(out.at[c, k], t_ref.at[k, c], keep.at[1]))

        own_copy(0).start()
        for c in range(n_c):
            own_copy(c).wait()

            @pl.loop(0, n_orb)
            def _(b):
                rows = pl.ds(pl.multiple_of(b * share, share), share)
                hi, mid, low = parts3(own_f[rows, :])
                part[rows, 0:n_q] = hi
                part[rows, n_q:2 * n_q] = mid
                part[rows, 2 * n_q:3 * n_q] = low

            if c + 1 < n_c:
                own_copy(c + 1).start()
            for r in range(1, n_aux):
                y_copy(c, r).wait_recv()
            if c > 0:
                for copy in keep_copies(c - 1):
                    copy.wait()

            def tile(h, start, width):
                rows = pl.ds(pl.multiple_of(h * half_rows, half_rows), half_rows)
                cols = pl.ds(start, width)
                hi = part[rows, 0:n_q]
                mid = part[rows, n_q:2 * n_q]
                low = part[rows, 2 * n_q:3 * n_q]
                left = jnp.concatenate([got[c, r, rows, :] for r in range(n_aux - 1)] + [hi, hi, hi, mid, mid, low], axis=1)
                res = jnp.dot(left, w_ref[:, cols], preferred_element_type=F32)
                res = res.reshape(n_orb // 2, share, width)
                first = pl.ds(h * (n_orb // 2), n_orb // 2)
                fit[first, :, cols] = res
                out[c, first, :, cols] = res.astype(BF16)

            @pl.loop(0, 2)
            def _(h):
                @pl.loop(0, n_p // WIDE)
                def _(n):
                    tile(h, pl.multiple_of(n * WIDE, WIDE), WIDE)
                if n_p % WIDE:
                    tile(h, n_p // WIDE * WIDE, n_p % WIDE)

            for r in range(1, n_orb):
                x_copy(c, r).start()
            for copy in keep_copies(c):
                copy.start()

        for copy in keep_copies(n_c - 1):
            copy.wait()
        for c in range(n_c):
            for r in range(1, n_aux):
                y_copy(c, r).wait_send()
            for r in range(1, n_orb):
                x_copy(c, r).wait()

    any_spec = pl.BlockSpec(memory_space=pl.ANY)
    return pl.pallas_call(
        kernel,
        out_shape=(jax.ShapeDtypeStruct((n_orb, n_c, share, n_p), BF16), jax.ShapeDtypeStruct((n_c, share, n_p), F32)),
        in_specs=[any_spec, any_spec, pl.BlockSpec(memory_space=pltpu.VMEM)],
        out_specs=(any_spec, any_spec),
        scratch_shapes=[
            pltpu.VMEM((n_c, n_aux - 1, n_rows, n_q), BF16),
            pltpu.VMEM((n_rows, n_q), F32),
            pltpu.VMEM((n_rows, 3 * n_q), BF16),
            pltpu.VMEM((n_orb, share, n_p), F32),
            pltpu.VMEM((n_c, n_orb, share, n_p), BF16),
            pltpu.SemaphoreType.DMA((n_c, n_aux - 1)), pltpu.SemaphoreType.DMA((n_c, n_aux - 1)),
            pltpu.SemaphoreType.DMA((n_c, n_orb - 1)), pltpu.SemaphoreType.DMA((n_c, n_orb - 1)),
            pltpu.SemaphoreType.DMA((1,)), pltpu.SemaphoreType.DMA((2,)),
        ],
        compiler_params=pltpu.CompilerParams(collective_id=0, has_side_effects=True, vmem_limit_bytes=62 * 2**20),
    )(x, own, weights)


def gram(t, mine):
    n_k, n_c, n_i, n_r, n_p = t.shape
    n_m, n_n = n_c * n_r, n_k * n_c * n_r

    def kernel(t_ref, mine_ref, o_ref, s_ref):
        all_t = t_ref[...].reshape(n_n, n_p)
        own = mine_ref[...].reshape(n_m, n_p)
        rest = own - own.astype(BF16).astype(F32)
        mid = rest.astype(BF16)
        low = (rest - mid.astype(F32)).astype(BF16)
        left = jnp.concatenate([all_t, mid, low], axis=0)
        nt = (((1,), (1,)), ((), ()))
        res = lax.dot_general(left, all_t, nt, preferred_element_type=F32)
        sq = lax.dot_general(mid, mid, nt, preferred_element_type=F32)

        @pl.when(pl.program_id(0) == 0)
        def _():
            o_ref[...] = res
            s_ref[...] = sq

        @pl.when(pl.program_id(0) > 0)
        def _():
            o_ref[...] += res
            s_ref[...] += sq

    return pl.pallas_call(
        kernel,
        grid=(n_i,),
        out_shape=(jax.ShapeDtypeStruct((n_n + 2 * n_m, n_n), F32), jax.ShapeDtypeStruct((n_m, n_m), F32)),
        in_specs=[pl.BlockSpec((n_k, n_c, 1, n_r, n_p), lambda i: (0, 0, i, 0, 0)),
                  pl.BlockSpec((n_c, 1, n_r, n_p), lambda i: (0, i, 0, 0))],
        out_specs=(pl.BlockSpec((n_n + 2 * n_m, n_n), lambda i: (0, 0)), pl.BlockSpec((n_m, n_m), lambda i: (0, 0))),
        compiler_params=pltpu.CompilerParams(vmem_limit_bytes=32 * 2**20),
    )(t, mine)


def solution(mesh):
    n_aux, n_orb = mesh.shape['aux'], mesh.shape['orb']

    def local_fock(ints, metric, orbitals):
        n_q, n_m, n_l = ints.shape
        n_d, _, n_i = orbitals.shape
        n_n, n_p = n_orb * n_m, n_aux * n_q
        n_c = n_m // ROWS_M
        pad_q, pad_p = round_up(n_q, LANES), round_up(n_p, LANES)
        j, k = lax.axis_index('aux'), lax.axis_index('orb')

        metric_pad = jnp.pad(metric, ((0, pad_q - n_q), (0, pad_p - n_p)))
        met = lax.all_gather(lax.reduce_precision(metric_pad, 8, 7).astype(BF16), 'aux', axis=0)
        met = jnp.concatenate([met, met], axis=0)
        met = lax.dynamic_slice_in_dim(met, j + 1, n_aux - 1, axis=0).reshape((n_aux - 1) * pad_q, pad_p)
        m_hi = lax.reduce_precision(metric_pad, 8, 7)
        m_mid = lax.reduce_precision(metric_pad - m_hi, 8, 7)
        m_low = metric_pad - m_hi - m_mid
        mets = [m.astype(BF16) for m in (m_hi, m_mid, m_low)]
        fit_w = jnp.concatenate([met] + mets + [mets[0], mets[1], mets[0]], axis=0)

        half = jnp.einsum('qml,dli->dimq', ints, orbitals, precision=PRECISE, preferred_element_type=F32)
        orb_rows = lax.dynamic_slice_in_dim(orbitals, k * n_m, n_m, axis=1)
        gamma = lax.psum(jnp.einsum('dimq,dmi->dq', half, orb_rows, precision=PRECISE), 'orb')
        gamma = lax.all_gather(gamma, 'aux', axis=1, tiled=True)
        gamma_fit = jnp.einsum('dq,pq->dp', gamma, metric, precision=PRECISE)
        weights = lax.psum_scatter(jnp.dot(gamma_fit, metric, precision=PRECISE), 'aux', scatter_dimension=1, tiled=True)
        coul = jnp.einsum('dq,qmn->dmn', weights, ints, precision=PRECISE)
        coul = lax.psum_scatter(coul, 'aux', scatter_dimension=2, tiled=True)

        half = half.reshape(n_d, n_i, n_c, ROWS_M, n_q).transpose(2, 0, 1, 3, 4)
        half = jnp.pad(half, ((0, 0),) * 4 + ((0, pad_q - n_q),)).reshape(n_c, n_d, n_i * ROWS_M, pad_q)
        own = lax.dynamic_index_in_dim(half, j, axis=1, keepdims=False)
        all_t, mine = fit_exchange(half.astype(BF16), own, fit_w, n_aux, n_orb)
        all_t = all_t.reshape(n_orb, n_c, n_i // n_orb, ROWS_M, pad_p)
        mine = mine.reshape(n_c, n_i // n_orb, ROWS_M, pad_p)
        exch, own_sq = gram(all_t, mine)
        cross = exch[n_n:n_n + n_m] + exch[n_n + n_m:]
        own_sq = lax.dynamic_update_slice_in_dim(jnp.zeros((n_m, n_n), F32), 0.5 * own_sq, k * n_m, axis=1)
        cross = lax.dynamic_update_slice_in_dim(jnp.zeros((n_n, n_n), F32), cross + own_sq, k * n_m, axis=0)
        exch = exch[:n_n] + cross + cross.T
        exch = lax.psum_scatter(exch, 'orb', scatter_dimension=0, tiled=True)
        exch = lax.all_to_all(exch.reshape(n_m, n_aux, n_n // n_aux), 'aux', 1, 0)
        return 2.0 * coul - exch.reshape(n_d, n_m, n_n // n_aux)

    return jax.shard_map(local_fock, mesh=mesh, in_specs=(P(('sys', 'aux'), 'orb', None), P(('sys', 'aux'), None), P('sys', None, None)), out_specs=P('sys', 'orb', 'aux'), check_vma=False)
```

```python
import jax
import jax.numpy as jnp
from jax import lax
from jax.experimental import pallas as pl
from jax.experimental.pallas import tpu as pltpu
from jax.sharding import PartitionSpec as P

PRECISE = lax.Precision.HIGHEST
F32 = jnp.float32
BF16 = jnp.bfloat16
MESH = pl.DeviceIdType.MESH
LANES = 128
WIDE = 256
SUB = 8
Q_TILE = 112


def round_up(n, to):
    return (n + to - 1) // to * to


def parts3(x):
    hi = x.astype(BF16)
    rest = x - hi.astype(F32)
    mid = rest.astype(BF16)
    return hi, mid, (rest - mid.astype(F32)).astype(BF16)


def split3(x):
    hi = lax.reduce_precision(x, 8, 7)
    mid = lax.reduce_precision(x - hi, 8, 7)
    return hi.astype(BF16), mid.astype(BF16), (x - hi - mid).astype(BF16)


def fit_exchange(ints, c_cat, c_rows, pick, weights, n_aux, n_orb, n_i):
    n_q, n_g, sub, n_l = ints.shape
    n_c = n_g // 2
    n_m = n_g * sub
    depth, n_p = weights.shape
    n_di = c_cat.shape[1]
    n_v = n_di // LANES
    n_d = n_aux
    pad_q = (n_q // Q_TILE) * LANES
    n_t = n_q // Q_TILE
    n_rows = n_i * 2 * sub
    share = n_rows // n_orb
    half_rows = n_rows // 2
    half_orb = n_orb // 2
    own_at = (n_aux - 1) * pad_q
    n_g_rows = pick.shape[0]

    def kernel(b_ref, c_ref, crow_ref, pick_ref, w_hbm, t_ref, mine_ref, j_ref,
               b_buf, w_ref, t_buf, temp, acc, send, part, got, fit, out, g_send, g_got, f_send, f_got, w_vec, w_smem,
               y_send, y_recv, x_send, x_recv, gx_send, gx_recv, gy_send, gy_recv, loc, keep):
        j, k = lax.axis_index('aux'), lax.axis_index('orb')
        load_w = pltpu.make_async_copy(w_hbm, w_ref, loc.at[1])

        def load_b(c):
            return pltpu.make_async_copy(b_ref.at[:, pl.ds(2 * c, 2)], b_buf, loc.at[0])

        load_b(0).start()
        load_w.start()
        barrier = pltpu.get_barrier_semaphore()
        for r in range(1, n_aux):
            pl.semaphore_signal(barrier, inc=1, device_id={'aux': lax.rem(j + r, n_aux)}, device_id_type=MESH)
        for r in range(1, n_orb):
            pl.semaphore_signal(barrier, inc=1, device_id={'orb': lax.rem(k + r, n_orb)}, device_id_type=MESH)

        def y_copy(c, r):
            to = lax.rem(j + n_aux - r, n_aux)
            return pltpu.make_async_remote_copy(
                src_ref=send.at[c % 2, to], dst_ref=got.at[c, r - 1], send_sem=y_send.at[c, r - 1],
                recv_sem=y_recv.at[c, r - 1], device_id={'aux': to}, device_id_type=MESH)

        def x_copy(c, r):
            to = lax.rem(k + r, n_orb)
            return pltpu.make_async_remote_copy(
                src_ref=out.at[c % 2, to], dst_ref=t_ref.at[k, c], send_sem=x_send.at[c, r - 1],
                recv_sem=x_recv.at[c, r - 1], device_id={'orb': to}, device_id_type=MESH)

        def gx_copy(r):
            return pltpu.make_async_remote_copy(
                src_ref=g_send, dst_ref=g_got.at[r - 1], send_sem=gx_send.at[r - 1], recv_sem=gx_recv.at[r - 1],
                device_id={'orb': lax.rem(k + r, n_orb)}, device_id_type=MESH)

        def gy_copy(r):
            return pltpu.make_async_remote_copy(
                src_ref=f_send, dst_ref=f_got.at[r - 1], send_sem=gy_send.at[r - 1], recv_sem=gy_recv.at[r - 1],
                device_id={'aux': lax.rem(j + r, n_aux)}, device_id_type=MESH)

        def keep_copies(c):
            return (pltpu.make_async_copy(fit.at[lax.rem(k, half_orb)], mine_ref.at[c], keep.at[0]),
                    pltpu.make_async_copy(out.at[c % 2, k], t_ref.at[k, c], keep.at[1]))

        acc[...] = jnp.zeros_like(acc)
        t_buf[:, Q_TILE * sub:, :] = jnp.zeros((n_v, (LANES - Q_TILE) * sub, LANES), F32)

        def transform(c):
            load_b(c).wait()
            if c >= 2:
                for r in range(1, n_aux):
                    y_copy(c - 2, r).wait_send()

            @pl.loop(0, n_t)
            def _(t):
                lanes = pl.ds(pl.multiple_of(t * LANES, LANES), LANES)

                @pl.loop(0, 2)
                def _(h):
                    q_rows = pl.ds(pl.multiple_of(t * Q_TILE, Q_TILE), Q_TILE)
                    hi, mid, low = parts3(b_buf[q_rows, h, :, :].reshape(Q_TILE * sub, n_l))
                    left = jnp.concatenate([hi, hi, hi, mid, mid, low], axis=1)
                    res = jnp.dot(left, c_ref[...], preferred_element_type=F32)
                    for v in range(n_v):
                        t_buf[v, 0:Q_TILE * sub, :] = res[:, v * LANES:(v + 1) * LANES]
                    for v in range(n_v):
                        part_di = slice(v * LANES, (v + 1) * LANES)
                        c_row = crow_ref[2 * c + h, :, part_di]
                        live = min(LANES, n_d * n_i - v * LANES)
                        total = acc[t, :, part_di]
                        for m in range(sub):
                            row = t_buf[v, pl.ds(m, LANES, stride=sub), :]
                            total += row * c_row[m:m + 1, :]
                            temp[h, pl.ds(v * LANES * sub + m, live, stride=sub), :] = row.T[:live, :]
                        acc[t, :, part_di] = total

                for d in range(n_d):
                    rows = pl.ds(d * n_i * sub, n_i * sub)
                    both = jnp.concatenate([temp[h, rows, :].reshape(n_i, sub, LANES) for h in range(2)], axis=1)
                    send[c % 2, d, :, lanes] = both.reshape(n_rows, LANES).astype(BF16)
                rows = pl.ds(pl.multiple_of(j * (n_i * sub), n_i * sub), n_i * sub)
                both = jnp.concatenate([temp[h, rows, :].reshape(n_i, sub, LANES) for h in range(2)], axis=1)
                for p, piece in enumerate(parts3(both.reshape(n_rows, LANES))):
                    part[c % 2, :, pl.ds(pl.multiple_of(p * pad_q + t * LANES, LANES), LANES)] = piece

            if c + 1 < n_c:
                load_b(c + 1).start()

        def fit_chunk(c):
            for r in range(1, n_aux):
                y_copy(c, r).wait_recv()
            if c > 0:
                for copy in keep_copies(c - 1):
                    copy.wait()
            if c >= 2:
                for r in range(1, n_orb):
                    x_copy(c - 2, r).wait_send()

            def tile(h, start, width):
                rows = pl.ds(pl.multiple_of(h * half_rows, half_rows), half_rows)
                cols = pl.ds(start, width)
                hi, mid, low = [part[c % 2, rows, p * pad_q:(p + 1) * pad_q] for p in range(3)]
                left = jnp.concatenate([got[c, r, rows, :] for r in range(n_aux - 1)] + [hi, hi, hi, mid, mid, low], axis=1)
                res = jnp.dot(left, w_ref[:, cols], preferred_element_type=F32).reshape(half_orb, share, width)
                out[c % 2, pl.ds(h * half_orb, half_orb), :, cols] = res.astype(BF16)

                @pl.when(h == k // half_orb)
                def _():
                    fit[:, :, cols] = res

            @pl.loop(0, 2)
            def _(h):
                @pl.loop(0, n_p // WIDE)
                def _(n):
                    tile(h, pl.multiple_of(n * WIDE, WIDE), WIDE)
                if n_p % WIDE:
                    tile(h, n_p // WIDE * WIDE, n_p % WIDE)

            for r in range(1, n_orb):
                x_copy(c, r).start()
            for copy in keep_copies(c):
                copy.start()

        def send_y(c):
            for r in range(1, n_aux):
                y_copy(c, r).start()

        nt = (((1,), (1,)), ((), ()))
        transform(0)
        pl.semaphore_wait(barrier, n_aux + n_orb - 2)
        send_y(0)
        transform(1)
        send_y(1)
        load_w.wait()
        fit_chunk(0)
        transform(2)
        send_y(2)
        load_b(0).start()
        g_send[...] = lax.dot_general(pick_ref[...], acc[...].reshape(n_t * LANES, n_di), nt, precision=PRECISE, preferred_element_type=F32)
        for r in range(1, n_orb):
            gx_copy(r).start()
        fit_chunk(1)
        for r in range(1, n_orb):
            gx_copy(r).wait()
        gamma = g_send[...]
        for r in range(1, n_orb):
            gamma += g_got[r - 1]
        hi, mid, low = parts3(gamma)
        left = jnp.concatenate([hi, hi, hi, mid, mid, low], axis=1)
        f_send[...] = jnp.dot(left, w_ref[own_at:, :], preferred_element_type=F32)
        for r in range(1, n_aux):
            gy_copy(r).start()
        for r in range(1, n_aux):
            gy_copy(r).wait()
        gamma_fit = f_send[...]
        for r in range(1, n_aux):
            gamma_fit += f_got[r - 1]
        hi, mid, low = parts3(gamma_fit)
        m_hi, m_mid, m_low = [w_ref[own_at + p * pad_q:own_at + (p + 1) * pad_q, :] for p in range(3)]
        by_hi = lax.dot_general(jnp.concatenate([hi, mid, low], axis=0), m_hi, nt, preferred_element_type=F32)
        by_mid = lax.dot_general(jnp.concatenate([hi, mid], axis=0), m_mid, nt, preferred_element_type=F32)
        by_low = lax.dot_general(hi, m_low, nt, preferred_element_type=F32)
        n = n_g_rows
        small = by_low + by_mid[n:] + by_hi[2 * n:]
        w_vec[...] = by_hi[:n] + ((by_hi[n:2 * n] + by_mid[:n]) + small)
        to_smem = pltpu.make_async_copy(w_vec, w_smem, loc.at[2])
        to_smem.start()
        to_smem.wait()
        for c in range(n_c):
            load_b(c).wait()
            for h in range(2):
                total = [jnp.zeros((sub, n_l), F32) for _ in range(n_d)]
                for t in range(n_t):
                    def some(s, total):
                        total = list(total)
                        for u in range(8):
                            q = s * 8 + u
                            block = b_buf[t * Q_TILE + q, h]
                            for d in range(n_d):
                                total[d] = total[d] + block * w_smem[d, t * LANES + q]
                        return tuple(total)
                    total = lax.fori_loop(0, Q_TILE // 8, some, tuple(total))
                for d in range(n_d):
                    j_ref[d, (2 * c + h) * sub:(2 * c + h + 1) * sub, :] = total[d]
            if c + 1 < n_c:
                load_b(c + 1).start()
        fit_chunk(2)

        for copy in keep_copies(n_c - 1):
            copy.wait()
        for c in range(n_c):
            for r in range(1, n_aux):
                if c >= n_c - 2:
                    y_copy(c, r).wait_send()
            for r in range(1, n_orb):
                if c >= n_c - 2:
                    x_copy(c, r).wait_send()
                x_copy(c, r).wait_recv()

    any_spec = pl.BlockSpec(memory_space=pl.ANY)
    vmem = pl.BlockSpec(memory_space=pltpu.VMEM)
    dma = pltpu.SemaphoreType.DMA
    return pl.pallas_call(
        kernel,
        out_shape=(jax.ShapeDtypeStruct((n_orb, n_c, share, n_p), BF16), jax.ShapeDtypeStruct((n_c, share, n_p), F32),
                   jax.ShapeDtypeStruct((n_d, n_m, n_l), F32)),
        in_specs=[any_spec, vmem, vmem, vmem, any_spec],
        out_specs=(any_spec, any_spec, vmem),
        scratch_shapes=[
            pltpu.VMEM((n_q, 2, sub, n_l), F32),
            pltpu.VMEM((depth, n_p), BF16),
            pltpu.VMEM((n_v, LANES * sub, LANES), F32),
            pltpu.VMEM((2, n_d * n_i * sub, LANES), F32),
            pltpu.VMEM((n_t, LANES, n_di), F32),
            pltpu.VMEM((2, n_d, n_rows, pad_q), BF16),
            pltpu.VMEM((2, n_rows, 3 * pad_q), BF16),
            pltpu.VMEM((n_c, n_aux - 1, n_rows, pad_q), BF16),
            pltpu.VMEM((half_orb, share, n_p), F32),
            pltpu.VMEM((2, n_orb, share, n_p), BF16),
            pltpu.VMEM((n_g_rows, pad_q), F32), pltpu.VMEM((n_orb - 1, n_g_rows, pad_q), F32),
            pltpu.VMEM((n_g_rows, n_p), F32), pltpu.VMEM((n_aux - 1, n_g_rows, n_p), F32),
            pltpu.VMEM((n_g_rows, pad_q), F32), pltpu.SMEM((n_g_rows, pad_q), F32),
            dma((n_c, n_aux - 1)), dma((n_c, n_aux - 1)), dma((n_c, n_orb - 1)), dma((n_c, n_orb - 1)),
            dma((n_orb - 1,)), dma((n_orb - 1,)), dma((n_aux - 1,)), dma((n_aux - 1,)),
            dma((3,)), dma((2,)),
        ],
        compiler_params=pltpu.CompilerParams(collective_id=0, has_side_effects=True, vmem_limit_bytes=67043328),
    )(ints, c_cat, c_rows, pick, weights)


def gram(t, mine):
    n_k, n_c, n_i, n_r, n_p = t.shape
    n_m, n_n = n_c * n_r, n_k * n_c * n_r

    def kernel(t_ref, mine_ref, o_ref, s_ref):
        all_t = t_ref[...].reshape(n_n, n_p)
        own = mine_ref[...].reshape(n_m, n_p)
        rest = own - own.astype(BF16).astype(F32)
        mid = rest.astype(BF16)
        low = (rest - mid.astype(F32)).astype(BF16)
        left = jnp.concatenate([all_t, mid, low], axis=0)
        nt = (((1,), (1,)), ((), ()))
        res = lax.dot_general(left, all_t, nt, preferred_element_type=F32)
        sq = lax.dot_general(mid, mid, nt, preferred_element_type=F32)

        @pl.when(pl.program_id(0) == 0)
        def _():
            o_ref[...] = res
            s_ref[...] = sq

        @pl.when(pl.program_id(0) > 0)
        def _():
            o_ref[...] += res
            s_ref[...] += sq

    return pl.pallas_call(
        kernel,
        grid=(n_i,),
        out_shape=(jax.ShapeDtypeStruct((n_n + 2 * n_m, n_n), F32), jax.ShapeDtypeStruct((n_m, n_m), F32)),
        in_specs=[pl.BlockSpec((n_k, n_c, 1, n_r, n_p), lambda i: (0, 0, i, 0, 0)),
                  pl.BlockSpec((n_c, 1, n_r, n_p), lambda i: (0, i, 0, 0))],
        out_specs=(pl.BlockSpec((n_n + 2 * n_m, n_n), lambda i: (0, 0)), pl.BlockSpec((n_m, n_m), lambda i: (0, 0))),
        compiler_params=pltpu.CompilerParams(vmem_limit_bytes=32 * 2**20),
    )(t, mine)


def solution(mesh):
    n_aux, n_orb = mesh.shape['aux'], mesh.shape['orb']

    def local_fock(ints, metric, orbitals):
        n_q, n_m, n_l = ints.shape
        n_d, _, n_i = orbitals.shape
        n_n, n_p = n_orb * n_m, n_aux * n_q
        n_c = n_m // (2 * SUB)
        pad_p = round_up(n_p, LANES)
        n_t = n_q // Q_TILE
        pad_q = n_t * LANES
        pad_di = round_up(n_d * n_i, LANES)
        j, k = lax.axis_index('aux'), lax.axis_index('orb')

        metric_pad = jnp.pad(metric.reshape(n_t, Q_TILE, n_p), ((0, 0), (0, LANES - Q_TILE), (0, pad_p - n_p))).reshape(pad_q, pad_p)
        m_hi, m_mid, m_low = split3(metric_pad)
        met = lax.all_gather(m_hi, 'aux', axis=0)
        met = jnp.concatenate([met, met], axis=0)
        met = lax.dynamic_slice_in_dim(met, j + 1, n_aux - 1, axis=0).reshape((n_aux - 1) * pad_q, pad_p)
        fit_w = jnp.concatenate([met, m_hi, m_mid, m_low, m_hi, m_mid, m_hi], axis=0)

        c_all = jnp.pad(orbitals.transpose(1, 0, 2).reshape(n_l, n_d * n_i), ((0, 0), (0, pad_di - n_d * n_i)))
        c_hi, c_mid, c_low = split3(c_all)
        c_cat = jnp.concatenate([c_hi, c_mid, c_low, c_hi, c_mid, c_hi], axis=0)
        c_rows = lax.dynamic_slice_in_dim(c_all, k * n_m, n_m, axis=0)
        lane = jnp.arange(pad_di)[None, :] // n_i
        pick = (lane == jnp.arange(2 * SUB)[:, None]).astype(F32)
        all_t, mine, coul = fit_exchange(ints.reshape(n_q, n_m // SUB, SUB, n_l), c_cat, c_rows.reshape(n_m // SUB, SUB, pad_di), pick, fit_w, n_aux, n_orb, n_i)
        coul = lax.psum_scatter(coul, 'aux', scatter_dimension=2, tiled=True)
        all_t = all_t.reshape(n_orb, n_c, n_i // n_orb, 2 * SUB, pad_p)
        mine = mine.reshape(n_c, n_i // n_orb, 2 * SUB, pad_p)
        exch, own_sq = gram(all_t, mine)
        cross = exch[n_n:n_n + n_m] + exch[n_n + n_m:]
        own_sq = lax.dynamic_update_slice_in_dim(jnp.zeros((n_m, n_n), F32), 0.5 * own_sq, k * n_m, axis=1)
        cross = lax.dynamic_update_slice_in_dim(jnp.zeros((n_n, n_n), F32), cross + own_sq, k * n_m, axis=0)
        exch = exch[:n_n] + cross + cross.T
        exch = lax.psum_scatter(exch, 'orb', scatter_dimension=0, tiled=True)
        exch = lax.all_to_all(exch.reshape(n_m, n_aux, n_n // n_aux), 'aux', 1, 0)
        return 2.0 * coul - exch.reshape(n_d, n_m, n_n // n_aux)

    return jax.shard_map(local_fock, mesh=mesh, in_specs=(P(('sys', 'aux'), 'orb', None), P(('sys', 'aux'), None), P('sys', None, None)), out_specs=P('sys', 'orb', 'aux'), check_vma=False)
```

```python
import jax
import jax.numpy as jnp
from jax import lax
from jax.experimental import pallas as pl
from jax.experimental.pallas import tpu as pltpu
from jax.sharding import PartitionSpec as P

PRECISE = lax.Precision.HIGHEST
F32 = jnp.float32
BF16 = jnp.bfloat16
MESH = pl.DeviceIdType.MESH
LANES = 128
WIDE = 256
SUB = 8
Q_TILE = 112


def round_up(n, to):
    return (n + to - 1) // to * to


def parts3(x):
    hi = x.astype(BF16)
    rest = x - hi.astype(F32)
    mid = rest.astype(BF16)
    return hi, mid, (rest - mid.astype(F32)).astype(BF16)


def split3(x):
    hi = lax.reduce_precision(x, 8, 7)
    mid = lax.reduce_precision(x - hi, 8, 7)
    return hi.astype(BF16), mid.astype(BF16), (x - hi - mid).astype(BF16)


def fit_exchange(ints, c_cat, c_rows, pick, weights, n_aux, n_orb, n_i):
    n_q, n_g, sub, n_l = ints.shape
    n_c = n_g // 2
    n_m = n_g * sub
    n_p = weights.shape[1]
    n_di = c_cat.shape[1]
    n_v = n_di // LANES
    n_d = n_aux
    pad_q = (n_q // Q_TILE) * LANES
    n_t = n_q // Q_TILE
    n_rows = n_i * 2 * sub
    half_rows = n_rows // 2
    share = half_rows // n_orb
    units = 2 * n_c
    slots = 4
    n_col = n_l // n_aux
    m_rows = pad_q // n_orb
    own_at = (n_aux - 1) * pad_q
    n_g_rows = pick.shape[0]

    def kernel(b_ref, c_ref, crow_ref, pick_ref, w_hbm, t_ref, mine_ref, j_ref,
               b_buf, w_ref, t_buf, temp, acc, send, part, got, fit, out, g_send, g_got, f_send, f_got, w_vec, w_smem, j_send, j_got,
               y_send, y_recv, x_send, x_recv, gx_send, gx_recv, gy_send, gy_recv, my_send, my_recv, mx_send, mx_recv,
               jy_send, jy_recv, loc, keep):
        j, k = lax.axis_index('aux'), lax.axis_index('orb')
        load_w = pltpu.make_async_copy(w_hbm, w_ref.at[pl.ds(own_at, w_hbm.shape[0])], loc.at[1])

        def load_b(c):
            return pltpu.make_async_copy(b_ref.at[:, pl.ds(2 * c, 2)], b_buf, loc.at[0])

        load_b(0).start()
        load_w.start()
        barrier = pltpu.get_barrier_semaphore()
        for r in range(1, n_aux):
            pl.semaphore_signal(barrier, inc=1, device_id={'aux': lax.rem(j + r, n_aux)}, device_id_type=MESH)
        for r in range(1, n_orb):
            pl.semaphore_signal(barrier, inc=1, device_id={'orb': lax.rem(k + r, n_orb)}, device_id_type=MESH)

        def cut(c, piece):
            if c == 0:
                return slice(None), pl.ds(piece * LANES, LANES)
            return pl.ds(piece * half_rows, half_rows), slice(None)

        def y_copy(c, r, piece):
            to = lax.rem(j + n_aux - r, n_aux)
            rows, lanes = cut(c, piece)
            return pltpu.make_async_remote_copy(
                src_ref=send.at[c % 2, to, rows, lanes], dst_ref=got.at[c, r - 1, rows, lanes], send_sem=y_send.at[c, r - 1, piece],
                recv_sem=y_recv.at[c, r - 1, piece], device_id={'aux': to}, device_id_type=MESH)

        def pieces(c):
            return range(n_t if c == 0 else 2)

        def x_copy(u, r):
            to = lax.rem(k + r, n_orb)
            return pltpu.make_async_remote_copy(
                src_ref=out.at[u % slots, to], dst_ref=t_ref.at[k, u], send_sem=x_send.at[u, r - 1],
                recv_sem=x_recv.at[u, r - 1], device_id={'orb': to}, device_id_type=MESH)

        def my_copy(r):
            to = lax.rem(j + n_aux - r, n_aux)
            return pltpu.make_async_remote_copy(
                src_ref=w_hbm.at[pl.ds(pl.multiple_of(k * m_rows, m_rows), m_rows)],
                dst_ref=w_ref.at[pl.ds(pl.multiple_of((r - 1) * pad_q + k * m_rows, m_rows), m_rows)],
                send_sem=my_send.at[r - 1], recv_sem=my_recv.at[r - 1], device_id={'aux': to}, device_id_type=MESH)

        def mx_copy(r, o):
            rows = w_ref.at[pl.ds(pl.multiple_of((r - 1) * pad_q + k * m_rows, m_rows), m_rows)]
            return pltpu.make_async_remote_copy(
                src_ref=rows, dst_ref=rows, send_sem=mx_send.at[r - 1, o - 1], recv_sem=mx_recv.at[r - 1, o - 1],
                device_id={'orb': lax.rem(k + o, n_orb)}, device_id_type=MESH)

        def jy_copy(r):
            to = lax.rem(j + n_aux - r, n_aux)
            return pltpu.make_async_remote_copy(
                src_ref=j_send.at[to], dst_ref=j_got.at[r - 1], send_sem=jy_send.at[r - 1], recv_sem=jy_recv.at[r - 1],
                device_id={'aux': to}, device_id_type=MESH)

        def gx_copy(r):
            return pltpu.make_async_remote_copy(
                src_ref=g_send, dst_ref=g_got.at[r - 1], send_sem=gx_send.at[r - 1], recv_sem=gx_recv.at[r - 1],
                device_id={'orb': lax.rem(k + r, n_orb)}, device_id_type=MESH)

        def gy_copy(r):
            return pltpu.make_async_remote_copy(
                src_ref=f_send, dst_ref=f_got.at[r - 1], send_sem=gy_send.at[r - 1], recv_sem=gy_recv.at[r - 1],
                device_id={'aux': lax.rem(j + r, n_aux)}, device_id_type=MESH)

        def keep_copies(u):
            return (pltpu.make_async_copy(fit.at[k], mine_ref.at[u], keep.at[0]),
                    pltpu.make_async_copy(out.at[u % slots, k], t_ref.at[k, u], keep.at[1]))

        acc[...] = jnp.zeros_like(acc)
        t_buf[:, Q_TILE * sub:, :] = jnp.zeros((n_v, (LANES - Q_TILE) * sub, LANES), F32)

        def transform(c):
            load_b(c).wait()
            if c >= 2:
                for r in range(1, n_aux):
                    for piece in pieces(c - 2):
                        y_copy(c - 2, r, piece).wait_send()

            def q_tile(t):
                lanes = pl.ds(pl.multiple_of(t * LANES, LANES), LANES)

                @pl.loop(0, 2)
                def _(h):
                    q_rows = pl.ds(pl.multiple_of(t * Q_TILE, Q_TILE), Q_TILE)
                    hi, mid, low = parts3(b_buf[q_rows, h, :, :].reshape(Q_TILE * sub, n_l))
                    left = jnp.concatenate([hi, hi, hi, mid, mid, low], axis=1)
                    res = jnp.dot(left, c_ref[...], preferred_element_type=F32)
                    for v in range(n_v):
                        t_buf[v, 0:Q_TILE * sub, :] = res[:, v * LANES:(v + 1) * LANES]
                    for v in range(n_v):
                        part_di = slice(v * LANES, (v + 1) * LANES)
                        c_row = crow_ref[2 * c + h, :, part_di]
                        live = min(LANES, n_d * n_i - v * LANES)
                        total = acc[t, :, part_di]
                        for m in range(sub):
                            row = t_buf[v, pl.ds(m, LANES, stride=sub), :]
                            total += row * c_row[m:m + 1, :]
                            temp[h, pl.ds(v * LANES * sub + m, live, stride=sub), :] = row.T[:live, :]
                        acc[t, :, part_di] = total

                for d in range(n_d):
                    rows = pl.ds(d * n_i * sub, n_i * sub)
                    both = jnp.concatenate([temp[h, rows, :].reshape(n_i, sub, LANES) for h in range(2)], axis=1)
                    send[c % 2, d, :, lanes] = both.reshape(n_rows, LANES).astype(BF16)
                rows = pl.ds(pl.multiple_of(j * (n_i * sub), n_i * sub), n_i * sub)
                both = jnp.concatenate([temp[h, rows, :].reshape(n_i, sub, LANES) for h in range(2)], axis=1)
                for p, piece in enumerate(parts3(both.reshape(n_rows, LANES))):
                    part[c % 2, :, pl.ds(pl.multiple_of(p * pad_q + t * LANES, LANES), LANES)] = piece

            if c == 0:
                for t in range(n_t):
                    q_tile(t)
                    for r in range(1, n_aux):
                        y_copy(c, r, t).start()
            else:
                pl.loop(0, n_t)(q_tile)
                for piece in pieces(c):
                    for r in range(1, n_aux):
                        y_copy(c, r, piece).start()
            if c + 1 < n_c:
                load_b(c + 1).start()

        def fit_chunk(c):
            for h in range(2):
                u = 2 * c + h
                for piece in (pieces(c) if h == 0 else ()) if c == 0 else (h,):
                    for r in range(1, n_aux):
                        y_copy(c, r, piece).wait_recv()
                if u > 0:
                    for copy in keep_copies(u - 1):
                        copy.wait()
                if u >= slots:
                    for r in range(1, n_orb):
                        x_copy(u - slots, r).wait_send()

                def tile(start, width):
                    rows = slice(h * half_rows, (h + 1) * half_rows)
                    cols = pl.ds(start, width)
                    hi, mid, low = [part[c % 2, rows, p * pad_q:(p + 1) * pad_q] for p in range(3)]
                    left = jnp.concatenate([got[c, r, rows, :] for r in range(n_aux - 1)] + [hi, hi, hi, mid, mid, low], axis=1)
                    res = jnp.dot(left, w_ref[:, cols], preferred_element_type=F32).reshape(n_orb, share, width)
                    out[u % slots, :, :, cols] = res.astype(BF16)
                    fit[:, :, cols] = res

                @pl.loop(0, n_p // WIDE)
                def _(n):
                    tile(pl.multiple_of(n * WIDE, WIDE), WIDE)
                if n_p % WIDE:
                    tile(n_p // WIDE * WIDE, n_p % WIDE)

                for r in range(1, n_orb):
                    x_copy(u, r).start()
                for copy in keep_copies(u):
                    copy.start()

        nt = (((1,), (1,)), ((), ()))
        pl.semaphore_wait(barrier, n_aux + n_orb - 2)
        for r in range(1, n_aux):
            my_copy(r).start()
        transform(0)
        for r in range(1, n_aux):
            my_copy(r).wait_recv()
            for o in range(1, n_orb):
                mx_copy(r, o).start()
        transform(1)
        load_w.wait()
        for r in range(1, n_aux):
            for o in range(1, n_orb):
                mx_copy(r, o).wait_recv()
        fit_chunk(0)
        transform(2)
        load_b(0).start()
        g_send[...] = lax.dot_general(pick_ref[...], acc[...].reshape(n_t * LANES, n_di), nt, precision=PRECISE, preferred_element_type=F32)
        for r in range(1, n_orb):
            gx_copy(r).start()
        fit_chunk(1)
        for r in range(1, n_orb):
            gx_copy(r).wait()
        gamma = g_send[...]
        for r in range(1, n_orb):
            gamma += g_got[r - 1]
        hi, mid, low = parts3(gamma)
        left = jnp.concatenate([hi, hi, hi, mid, mid, low], axis=1)
        f_send[...] = jnp.dot(left, w_ref[own_at:, :], preferred_element_type=F32)
        for r in range(1, n_aux):
            gy_copy(r).start()
        for r in range(1, n_aux):
            gy_copy(r).wait()
        gamma_fit = f_send[...]
        for r in range(1, n_aux):
            gamma_fit += f_got[r - 1]
        hi, mid, low = parts3(gamma_fit)
        m_hi, m_mid, m_low = [w_ref[own_at + p * pad_q:own_at + (p + 1) * pad_q, :] for p in range(3)]
        by_hi = lax.dot_general(jnp.concatenate([hi, mid, low], axis=0), m_hi, nt, preferred_element_type=F32)
        by_mid = lax.dot_general(jnp.concatenate([hi, mid], axis=0), m_mid, nt, preferred_element_type=F32)
        by_low = lax.dot_general(hi, m_low, nt, preferred_element_type=F32)
        n = n_g_rows
        small = by_low + by_mid[n:] + by_hi[2 * n:]
        w_vec[...] = by_hi[:n] + ((by_hi[n:2 * n] + by_mid[:n]) + small)
        to_smem = pltpu.make_async_copy(w_vec, w_smem, loc.at[2])
        to_smem.start()
        to_smem.wait()
        for c in range(n_c):
            load_b(c).wait()
            for h in range(2):
                total = [jnp.zeros((sub, n_l), F32) for _ in range(n_d)]
                for t in range(n_t):
                    def some(s, total):
                        total = list(total)
                        for u in range(8):
                            q = s * 8 + u
                            block = b_buf[t * Q_TILE + q, h]
                            for d in range(n_d):
                                total[d] = total[d] + block * w_smem[d, t * LANES + q]
                        return tuple(total)
                    total = lax.fori_loop(0, Q_TILE // 8, some, tuple(total))
                for d in range(n_d):
                    for to in range(n_aux):
                        j_send[to, d, (2 * c + h) * sub:(2 * c + h + 1) * sub, :] = total[d][:, to * n_col:(to + 1) * n_col]
            if c + 1 < n_c:
                load_b(c + 1).start()
        for r in range(1, n_aux):
            jy_copy(r).start()
        fit_chunk(2)
        for r in range(1, n_aux):
            jy_copy(r).wait()
        coul = j_send[j]
        for r in range(1, n_aux):
            coul += j_got[r - 1]
        j_ref[...] = coul

        for copy in keep_copies(units - 1):
            copy.wait()
        for r in range(1, n_aux):
            my_copy(r).wait_send()
            for o in range(1, n_orb):
                mx_copy(r, o).wait_send()
            for c in range(n_c - 2, n_c):
                for piece in pieces(c):
                    y_copy(c, r, piece).wait_send()
        for u in range(units):
            for r in range(1, n_orb):
                if u >= units - slots:
                    x_copy(u, r).wait_send()
                x_copy(u, r).wait_recv()

    any_spec = pl.BlockSpec(memory_space=pl.ANY)
    vmem = pl.BlockSpec(memory_space=pltpu.VMEM)
    dma = pltpu.SemaphoreType.DMA
    return pl.pallas_call(
        kernel,
        out_shape=(jax.ShapeDtypeStruct((n_orb, units, share, n_p), BF16), jax.ShapeDtypeStruct((units, share, n_p), F32),
                   jax.ShapeDtypeStruct((n_d, n_m, n_col), F32)),
        in_specs=[any_spec, vmem, vmem, vmem, any_spec],
        out_specs=(any_spec, any_spec, vmem),
        scratch_shapes=[
            pltpu.VMEM((n_q, 2, sub, n_l), F32),
            pltpu.VMEM((own_at + weights.shape[0], n_p), BF16),
            pltpu.VMEM((n_v, LANES * sub, LANES), F32),
            pltpu.VMEM((2, n_d * n_i * sub, LANES), F32),
            pltpu.VMEM((n_t, LANES, n_di), F32),
            pltpu.VMEM((2, n_d, n_rows, pad_q), BF16),
            pltpu.VMEM((2, n_rows, 3 * pad_q), BF16),
            pltpu.VMEM((n_c, n_aux - 1, n_rows, pad_q), BF16),
            pltpu.VMEM((n_orb, share, n_p), F32),
            pltpu.VMEM((slots, n_orb, share, n_p), BF16),
            pltpu.VMEM((n_g_rows, pad_q), F32), pltpu.VMEM((n_orb - 1, n_g_rows, pad_q), F32),
            pltpu.VMEM((n_g_rows, n_p), F32), pltpu.VMEM((n_aux - 1, n_g_rows, n_p), F32),
            pltpu.VMEM((n_g_rows, pad_q), F32), pltpu.SMEM((n_g_rows, pad_q), F32),
            pltpu.VMEM((n_aux, n_d, n_m, n_col), F32), pltpu.VMEM((n_aux - 1, n_d, n_m, n_col), F32),
            dma((n_c, n_aux - 1, n_t)), dma((n_c, n_aux - 1, n_t)), dma((units, n_orb - 1)), dma((units, n_orb - 1)),
            dma((n_orb - 1,)), dma((n_orb - 1,)), dma((n_aux - 1,)), dma((n_aux - 1,)),
            dma((n_aux - 1,)), dma((n_aux - 1,)), dma((n_aux - 1, n_orb - 1)), dma((n_aux - 1, n_orb - 1)),
            dma((n_aux - 1,)), dma((n_aux - 1,)),
            dma((3,)), dma((2,)),
        ],
        compiler_params=pltpu.CompilerParams(collective_id=0, has_side_effects=True, vmem_limit_bytes=67043328),
    )(ints, c_cat, c_rows, pick, weights)


def gram(t, mine, coul, n_aux):
    n_k, n_c, n_i, n_r, n_p = t.shape
    n_m, n_n = n_c * n_r, n_k * n_c * n_r
    n_col = n_n // n_aux

    def kernel(t_hbm, mine_ref, coul_ref, g_ref, t_ref, acc, sq, side, k_send, k_got, c_send, c_got,
               load, ks_send, ks_recv, cs_send, cs_recv):
        j, k = lax.axis_index('aux'), lax.axis_index('orb')

        def load_t(i):
            return pltpu.make_async_copy(t_hbm.at[:, :, i], t_ref.at[i], load.at[i])

        def k_copy(r):
            to = lax.rem(k + r, n_k)
            return pltpu.make_async_remote_copy(
                src_ref=k_send.at[to], dst_ref=k_got.at[r - 1], send_sem=ks_send.at[r - 1], recv_sem=ks_recv.at[r - 1],
                device_id={'orb': to}, device_id_type=MESH)

        def c_copy(r):
            to = lax.rem(j + n_aux - r, n_aux)
            return pltpu.make_async_remote_copy(
                src_ref=c_send.at[to], dst_ref=c_got.at[r - 1], send_sem=cs_send.at[r - 1], recv_sem=cs_recv.at[r - 1],
                device_id={'aux': to}, device_id_type=MESH)

        for i in range(n_i):
            load_t(i).start()
        barrier = pltpu.get_barrier_semaphore()
        for r in range(1, n_aux):
            pl.semaphore_signal(barrier, inc=1, device_id={'aux': lax.rem(j + r, n_aux)}, device_id_type=MESH)
        for r in range(1, n_k):
            pl.semaphore_signal(barrier, inc=1, device_id={'orb': lax.rem(k + r, n_k)}, device_id_type=MESH)
        acc[...] = jnp.zeros_like(acc)
        sq[...] = jnp.zeros_like(sq)
        nt = (((1,), (1,)), ((), ()))

        @pl.loop(0, n_i)
        def _(i):
            load_t(i).wait()
            all_t = t_ref[i].reshape(n_n, n_p)
            own = mine_ref[:, i].reshape(n_m, n_p)
            _, mid, low = parts3(own)
            left = jnp.concatenate([all_t, mid, low], axis=0)
            acc[...] += lax.dot_general(left, all_t, nt, preferred_element_type=F32)
            sq[...] += lax.dot_general(mid, mid, nt, preferred_element_type=F32)

        put = lax.broadcasted_iota(jnp.int32, (n_m, n_n), 1) == lax.broadcasted_iota(jnp.int32, (n_m, n_n), 0) + k * n_m
        own_sq = jnp.dot(0.5 * sq[...], put.astype(F32), precision=PRECISE, preferred_element_type=F32)
        side[...] = jnp.zeros_like(side)
        side[pl.ds(pl.multiple_of(k * n_m, 8), n_m), :] = acc[n_n:n_n + n_m, :] + acc[n_n + n_m:, :] + own_sq
        k_send[...] = (acc[:n_n, :] + side[...] + side[...].T).reshape(n_k, n_m, n_n)
        pl.semaphore_wait(barrier, n_aux + n_k - 2)
        for r in range(1, n_k):
            k_copy(r).start()
        for r in range(1, n_k):
            k_copy(r).wait()
        total = k_send[k]
        for r in range(1, n_k):
            total += k_got[r - 1]
        for to in range(n_aux):
            c_send[to] = total[:, to * n_col:(to + 1) * n_col]
        for r in range(1, n_aux):
            c_copy(r).start()
        g_ref[j] = 2.0 * coul_ref[j] - c_send[j]
        for r in range(1, n_aux):
            c_copy(r).wait()
            d = lax.rem(j + r, n_aux)
            g_ref[d] = 2.0 * coul_ref[d] - c_got[r - 1]

    any_spec = pl.BlockSpec(memory_space=pl.ANY)
    vmem = pl.BlockSpec(memory_space=pltpu.VMEM)
    dma = pltpu.SemaphoreType.DMA
    return pl.pallas_call(
        kernel,
        out_shape=jax.ShapeDtypeStruct((n_aux, n_m, n_col), F32),
        in_specs=[any_spec, vmem, vmem],
        out_specs=vmem,
        scratch_shapes=[
            pltpu.VMEM((n_i, n_k, n_c, n_r, n_p), BF16),
            pltpu.VMEM((n_n + 2 * n_m, n_n), F32), pltpu.VMEM((n_m, n_m), F32), pltpu.VMEM((n_n, n_n), F32),
            pltpu.VMEM((n_k, n_m, n_n), F32), pltpu.VMEM((n_k - 1, n_m, n_n), F32),
            pltpu.VMEM((n_aux, n_m, n_col), F32), pltpu.VMEM((n_aux - 1, n_m, n_col), F32),
            dma((n_i,)), dma((n_k - 1,)), dma((n_k - 1,)), dma((n_aux - 1,)), dma((n_aux - 1,)),
        ],
        compiler_params=pltpu.CompilerParams(collective_id=1, has_side_effects=True, vmem_limit_bytes=40 * 2**20),
    )(t, mine, coul)


def solution(mesh):
    n_aux, n_orb = mesh.shape['aux'], mesh.shape['orb']

    def local_fock(ints, metric, orbitals):
        n_q, n_m, n_l = ints.shape
        n_d, _, n_i = orbitals.shape
        n_p = n_aux * n_q
        n_c = n_m // (2 * SUB)
        pad_p = round_up(n_p, LANES)
        n_t = n_q // Q_TILE
        pad_q = n_t * LANES
        pad_di = round_up(n_d * n_i, LANES)
        k = lax.axis_index('orb')

        metric_pad = jnp.pad(metric.reshape(n_t, Q_TILE, n_p), ((0, 0), (0, LANES - Q_TILE), (0, pad_p - n_p))).reshape(pad_q, pad_p)
        m_hi, m_mid, m_low = split3(metric_pad)
        fit_w = jnp.concatenate([m_hi, m_mid, m_low, m_hi, m_mid, m_hi], axis=0)

        c_all = jnp.pad(orbitals.transpose(1, 0, 2).reshape(n_l, n_d * n_i), ((0, 0), (0, pad_di - n_d * n_i)))
        c_hi, c_mid, c_low = split3(c_all)
        c_cat = jnp.concatenate([c_hi, c_mid, c_low, c_hi, c_mid, c_hi], axis=0)
        c_rows = lax.dynamic_slice_in_dim(c_all, k * n_m, n_m, axis=0)
        lane = jnp.arange(pad_di)[None, :] // n_i
        pick = (lane == jnp.arange(2 * SUB)[:, None]).astype(F32)
        all_t, mine, coul = fit_exchange(ints.reshape(n_q, n_m // SUB, SUB, n_l), c_cat, c_rows.reshape(n_m // SUB, SUB, pad_di), pick, fit_w, n_aux, n_orb, n_i)
        all_t = all_t.reshape(n_orb, n_c, n_i // n_orb, 2 * SUB, pad_p)
        mine = mine.reshape(n_c, n_i // n_orb, 2 * SUB, pad_p)
        return gram(all_t, mine, coul, n_aux)

    return jax.shard_map(local_fock, mesh=mesh, in_specs=(P(('sys', 'aux'), 'orb', None), P(('sys', 'aux'), None), P('sys', None, None)), out_specs=P('sys', 'orb', 'aux'), check_vma=False)
```

```python
import jax
import jax.numpy as jnp
from jax import lax
from jax.experimental import pallas as pl
from jax.experimental.pallas import tpu as pltpu
from jax.sharding import PartitionSpec as P

PRECISE = lax.Precision.HIGHEST
F32 = jnp.float32
BF16 = jnp.bfloat16
MESH = pl.DeviceIdType.MESH
LANES = 128
WIDE = 256
SUB = 8
Q_TILE = 112


def round_up(n, to):
    return (n + to - 1) // to * to


def parts3(x):
    hi = x.astype(BF16)
    rest = x - hi.astype(F32)
    mid = rest.astype(BF16)
    return hi, mid, (rest - mid.astype(F32)).astype(BF16)


def split3(x):
    hi = lax.reduce_precision(x, 8, 7)
    mid = lax.reduce_precision(x - hi, 8, 7)
    return hi.astype(BF16), mid.astype(BF16), (x - hi - mid).astype(BF16)


def fit_exchange(ints, c_cat, c_rows, pick, weights, n_aux, n_orb, n_i):
    n_q, n_g, sub, n_l = ints.shape
    n_c = n_g // 2
    n_m = n_g * sub
    n_p = weights.shape[1]
    n_di = c_cat.shape[1]
    n_v = n_di // LANES
    n_d = n_aux
    pad_q = (n_q // Q_TILE) * LANES
    n_t = n_q // Q_TILE
    n_rows = n_i * 2 * sub
    half_rows = n_rows // 2
    share = half_rows // n_orb
    units = 2 * n_c
    slots = 4
    n_col = n_l // n_aux
    m_rows = pad_q // n_orb
    own_at = (n_aux - 1) * pad_q
    n_g_rows = pick.shape[0]

    def kernel(b_ref, c_ref, crow_ref, pick_ref, w_hbm, t_ref, mine_ref, j_ref,
               b_buf, w_ref, t_buf, temp, acc, send, part, got, fit, out, g_send, g_got, f_send, f_got, w_vec, w_smem, j_send, j_got,
               y_send, y_recv, x_send, x_recv, gx_send, gx_recv, gy_send, gy_recv, my_send, my_recv, mx_send, mx_recv,
               jy_send, jy_recv, loc, keep):
        j, k = lax.axis_index('aux'), lax.axis_index('orb')
        load_w = pltpu.make_async_copy(w_hbm, w_ref.at[pl.ds(own_at, w_hbm.shape[0])], loc.at[1])

        def load_b(c):
            return pltpu.make_async_copy(b_ref.at[:, pl.ds(2 * c, 2)], b_buf, loc.at[0])

        load_b(0).start()
        load_w.start()
        barrier = pltpu.get_barrier_semaphore()
        for r in range(1, n_aux):
            pl.semaphore_signal(barrier, inc=1, device_id={'aux': lax.rem(j + r, n_aux)}, device_id_type=MESH)
        for r in range(1, n_orb):
            pl.semaphore_signal(barrier, inc=1, device_id={'orb': lax.rem(k + r, n_orb)}, device_id_type=MESH)

        def cut(c, piece):
            if piece >= 2:
                return pl.ds(0, half_rows), pl.ds((piece - 2) * LANES, LANES)
            return pl.ds(piece * half_rows, half_rows), slice(None)

        def y_copy(c, r, piece):
            to = lax.rem(j + n_aux - r, n_aux)
            rows, lanes = cut(c, piece)
            return pltpu.make_async_remote_copy(
                src_ref=send.at[c % 2, to, rows, lanes], dst_ref=got.at[c, r - 1, rows, lanes], send_sem=y_send.at[c, r - 1, piece],
                recv_sem=y_recv.at[c, r - 1, piece], device_id={'aux': to}, device_id_type=MESH)

        def pieces(c, h):
            return tuple(range(2, 2 + n_t)) if c == 0 and h == 0 else (h,)

        def x_copy(u, r):
            to = lax.rem(k + r, n_orb)
            return pltpu.make_async_remote_copy(
                src_ref=out.at[u % slots, to], dst_ref=t_ref.at[k, u], send_sem=x_send.at[u, r - 1],
                recv_sem=x_recv.at[u, r - 1], device_id={'orb': to}, device_id_type=MESH)

        def my_copy(r):
            to = lax.rem(j + n_aux - r, n_aux)
            return pltpu.make_async_remote_copy(
                src_ref=w_hbm.at[pl.ds(pl.multiple_of(k * m_rows, m_rows), m_rows)],
                dst_ref=w_ref.at[pl.ds(pl.multiple_of((r - 1) * pad_q + k * m_rows, m_rows), m_rows)],
                send_sem=my_send.at[r - 1], recv_sem=my_recv.at[r - 1], device_id={'aux': to}, device_id_type=MESH)

        def mx_copy(r, o):
            rows = w_ref.at[pl.ds(pl.multiple_of((r - 1) * pad_q + k * m_rows, m_rows), m_rows)]
            return pltpu.make_async_remote_copy(
                src_ref=rows, dst_ref=rows, send_sem=mx_send.at[r - 1, o - 1], recv_sem=mx_recv.at[r - 1, o - 1],
                device_id={'orb': lax.rem(k + o, n_orb)}, device_id_type=MESH)

        def jy_copy(r):
            to = lax.rem(j + n_aux - r, n_aux)
            return pltpu.make_async_remote_copy(
                src_ref=j_send.at[to], dst_ref=j_got.at[r - 1], send_sem=jy_send.at[r - 1], recv_sem=jy_recv.at[r - 1],
                device_id={'aux': to}, device_id_type=MESH)

        def gx_copy(r):
            return pltpu.make_async_remote_copy(
                src_ref=g_send, dst_ref=g_got.at[r - 1], send_sem=gx_send.at[r - 1], recv_sem=gx_recv.at[r - 1],
                device_id={'orb': lax.rem(k + r, n_orb)}, device_id_type=MESH)

        def gy_copy(r):
            return pltpu.make_async_remote_copy(
                src_ref=f_send, dst_ref=f_got.at[r - 1], send_sem=gy_send.at[r - 1], recv_sem=gy_recv.at[r - 1],
                device_id={'aux': lax.rem(j + r, n_aux)}, device_id_type=MESH)

        def keep_copies(u):
            return (pltpu.make_async_copy(fit.at[k], mine_ref.at[u], keep.at[0]),
                    pltpu.make_async_copy(out.at[u % slots, k], t_ref.at[k, u], keep.at[1]))

        acc[...] = jnp.zeros_like(acc)
        t_buf[:, Q_TILE * sub:, :] = jnp.zeros((n_v, (LANES - Q_TILE) * sub, LANES), F32)

        def transform(c):
            load_b(c).wait()
            if c >= 2:
                for r in range(1, n_aux):
                    for piece in pieces(c - 2, 0) + pieces(c - 2, 1):
                        y_copy(c - 2, r, piece).wait_send()

            def q_tile(t):
                lanes = pl.ds(pl.multiple_of(t * LANES, LANES), LANES)

                @pl.loop(0, 2)
                def _(h):
                    q_rows = pl.ds(pl.multiple_of(t * Q_TILE, Q_TILE), Q_TILE)
                    hi, mid, low = parts3(b_buf[q_rows, h, :, :].reshape(Q_TILE * sub, n_l))
                    left = jnp.concatenate([hi, hi, hi, mid, mid, low], axis=1)
                    res = jnp.dot(left, c_ref[...], preferred_element_type=F32)
                    for v in range(n_v):
                        t_buf[v, 0:Q_TILE * sub, :] = res[:, v * LANES:(v + 1) * LANES]
                    for v in range(n_v):
                        part_di = slice(v * LANES, (v + 1) * LANES)
                        c_row = crow_ref[2 * c + h, :, part_di]
                        live = min(LANES, n_d * n_i - v * LANES)
                        total = acc[t, :, part_di]
                        for m in range(sub):
                            row = t_buf[v, pl.ds(m, LANES, stride=sub), :]
                            total += row * c_row[m:m + 1, :]
                            temp[h, pl.ds(v * LANES * sub + m, live, stride=sub), :] = row.T[:live, :]
                        acc[t, :, part_di] = total

                for d in range(n_d):
                    rows = pl.ds(d * n_i * sub, n_i * sub)
                    both = jnp.concatenate([temp[h, rows, :].reshape(n_i, sub, LANES) for h in range(2)], axis=1)
                    send[c % 2, d, :, lanes] = both.reshape(n_rows, LANES).astype(BF16)
                rows = pl.ds(pl.multiple_of(j * (n_i * sub), n_i * sub), n_i * sub)
                both = jnp.concatenate([temp[h, rows, :].reshape(n_i, sub, LANES) for h in range(2)], axis=1)
                for p, piece in enumerate(parts3(both.reshape(n_rows, LANES))):
                    part[c % 2, :, pl.ds(pl.multiple_of(p * pad_q + t * LANES, LANES), LANES)] = piece

            if c == 0:
                for t in range(n_t):
                    q_tile(t)
                    for r in range(1, n_aux):
                        y_copy(c, r, 2 + t).start()
                    if t == 0:
                        for r in range(1, n_aux):
                            my_copy(r).wait_recv()
                            for o in range(1, n_orb):
                                mx_copy(r, o).start()
                for r in range(1, n_aux):
                    y_copy(c, r, 1).start()
            else:
                pl.loop(0, n_t)(q_tile)
                for piece in (0, 1):
                    for r in range(1, n_aux):
                        y_copy(c, r, piece).start()
            if c + 1 < n_c:
                load_b(c + 1).start()

        def fit_half(c, h):
            u = 2 * c + h
            for piece in pieces(c, h):
                for r in range(1, n_aux):
                    y_copy(c, r, piece).wait_recv()
            if u > 0:
                for copy in keep_copies(u - 1):
                    copy.wait()
            if u >= slots:
                for r in range(1, n_orb):
                    x_copy(u - slots, r).wait_send()

            def tile(start, width):
                rows = slice(h * half_rows, (h + 1) * half_rows)
                cols = pl.ds(start, width)
                hi, mid, low = [part[c % 2, rows, p * pad_q:(p + 1) * pad_q] for p in range(3)]
                left = jnp.concatenate([got[c, r, rows, :] for r in range(n_aux - 1)] + [hi, hi, hi, mid, mid, low], axis=1)
                res = jnp.dot(left, w_ref[:, cols], preferred_element_type=F32).reshape(n_orb, share, width)
                out[u % slots, :, :, cols] = res.astype(BF16)
                fit[:, :, cols] = res

            @pl.loop(0, n_p // WIDE)
            def _(n):
                tile(pl.multiple_of(n * WIDE, WIDE), WIDE)
            if n_p % WIDE:
                tile(n_p // WIDE * WIDE, n_p % WIDE)

            for r in range(1, n_orb):
                x_copy(u, r).start()
            for copy in keep_copies(u):
                copy.start()

        nt = (((1,), (1,)), ((), ()))
        pl.semaphore_wait(barrier, n_aux + n_orb - 2)
        for r in range(1, n_aux):
            my_copy(r).start()
        transform(0)
        transform(1)
        load_w.wait()
        for r in range(1, n_aux):
            for o in range(1, n_orb):
                mx_copy(r, o).wait_recv()
        fit_half(0, 0)
        fit_half(0, 1)
        transform(2)
        load_b(0).start()
        g_send[...] = lax.dot_general(pick_ref[...], acc[...].reshape(n_t * LANES, n_di), nt, precision=PRECISE, preferred_element_type=F32)
        for r in range(1, n_orb):
            gx_copy(r).start()
        fit_half(1, 0)
        for r in range(1, n_orb):
            gx_copy(r).wait()
        gamma = g_send[...]
        for r in range(1, n_orb):
            gamma += g_got[r - 1]
        hi, mid, low = parts3(gamma)
        left = jnp.concatenate([hi, hi, hi, mid, mid, low], axis=1)
        f_send[...] = jnp.dot(left, w_ref[own_at:, :], preferred_element_type=F32)
        for r in range(1, n_aux):
            gy_copy(r).start()
        fit_half(1, 1)
        for r in range(1, n_aux):
            gy_copy(r).wait()
        gamma_fit = f_send[...]
        for r in range(1, n_aux):
            gamma_fit += f_got[r - 1]
        hi, mid, low = parts3(gamma_fit)
        m_hi, m_mid, m_low = [w_ref[own_at + p * pad_q:own_at + (p + 1) * pad_q, :] for p in range(3)]
        by_hi = lax.dot_general(jnp.concatenate([hi, mid, low], axis=0), m_hi, nt, preferred_element_type=F32)
        by_mid = lax.dot_general(jnp.concatenate([hi, mid], axis=0), m_mid, nt, preferred_element_type=F32)
        by_low = lax.dot_general(hi, m_low, nt, preferred_element_type=F32)
        n = n_g_rows
        small = by_low + by_mid[n:] + by_hi[2 * n:]
        w_vec[...] = by_hi[:n] + ((by_hi[n:2 * n] + by_mid[:n]) + small)
        to_smem = pltpu.make_async_copy(w_vec, w_smem, loc.at[2])
        to_smem.start()
        to_smem.wait()
        for c in range(n_c):
            if c > 0:
                fit_half(2, c - 1)
            load_b(c).wait()
            for h in range(2):
                total = [jnp.zeros((sub, n_l), F32) for _ in range(n_d)]
                for t in range(n_t):
                    def some(s, total):
                        total = list(total)
                        for u in range(8):
                            q = s * 8 + u
                            block = b_buf[t * Q_TILE + q, h]
                            for d in range(n_d):
                                total[d] = total[d] + block * w_smem[d, t * LANES + q]
                        return tuple(total)
                    total = lax.fori_loop(0, Q_TILE // 8, some, tuple(total))
                for d in range(n_d):
                    for to in range(n_aux):
                        j_send[to, d, (2 * c + h) * sub:(2 * c + h + 1) * sub, :] = total[d][:, to * n_col:(to + 1) * n_col]
            if c + 1 < n_c:
                load_b(c + 1).start()
        for r in range(1, n_aux):
            jy_copy(r).start()
        for r in range(1, n_aux):
            jy_copy(r).wait()
        coul = j_send[j]
        for r in range(1, n_aux):
            coul += j_got[r - 1]
        j_ref[...] = coul

        for copy in keep_copies(units - 1):
            copy.wait()
        for r in range(1, n_aux):
            my_copy(r).wait_send()
            for o in range(1, n_orb):
                mx_copy(r, o).wait_send()
            for c in range(n_c - 2, n_c):
                for piece in pieces(c, 0) + pieces(c, 1):
                    y_copy(c, r, piece).wait_send()
        for u in range(units):
            for r in range(1, n_orb):
                if u >= units - slots:
                    x_copy(u, r).wait_send()
                x_copy(u, r).wait_recv()

    any_spec = pl.BlockSpec(memory_space=pl.ANY)
    vmem = pl.BlockSpec(memory_space=pltpu.VMEM)
    dma = pltpu.SemaphoreType.DMA
    return pl.pallas_call(
        kernel,
        out_shape=(jax.ShapeDtypeStruct((n_orb, units, share, n_p), BF16), jax.ShapeDtypeStruct((units, share, n_p), F32),
                   jax.ShapeDtypeStruct((n_d, n_m, n_col), F32)),
        in_specs=[any_spec, vmem, vmem, vmem, any_spec],
        out_specs=(any_spec, any_spec, vmem),
        scratch_shapes=[
            pltpu.VMEM((n_q, 2, sub, n_l), F32),
            pltpu.VMEM((own_at + weights.shape[0], n_p), BF16),
            pltpu.VMEM((n_v, LANES * sub, LANES), F32),
            pltpu.VMEM((2, n_d * n_i * sub, LANES), F32),
            pltpu.VMEM((n_t, LANES, n_di), F32),
            pltpu.VMEM((2, n_d, n_rows, pad_q), BF16),
            pltpu.VMEM((2, n_rows, 3 * pad_q), BF16),
            pltpu.VMEM((n_c, n_aux - 1, n_rows, pad_q), BF16),
            pltpu.VMEM((n_orb, share, n_p), F32),
            pltpu.VMEM((slots, n_orb, share, n_p), BF16),
            pltpu.VMEM((n_g_rows, pad_q), F32), pltpu.VMEM((n_orb - 1, n_g_rows, pad_q), F32),
            pltpu.VMEM((n_g_rows, n_p), F32), pltpu.VMEM((n_aux - 1, n_g_rows, n_p), F32),
            pltpu.VMEM((n_g_rows, pad_q), F32), pltpu.SMEM((n_g_rows, pad_q), F32),
            pltpu.VMEM((n_aux, n_d, n_m, n_col), F32), pltpu.VMEM((n_aux - 1, n_d, n_m, n_col), F32),
            dma((n_c, n_aux - 1, 2 + n_t)), dma((n_c, n_aux - 1, 2 + n_t)), dma((units, n_orb - 1)), dma((units, n_orb - 1)),
            dma((n_orb - 1,)), dma((n_orb - 1,)), dma((n_aux - 1,)), dma((n_aux - 1,)),
            dma((n_aux - 1,)), dma((n_aux - 1,)), dma((n_aux - 1, n_orb - 1)), dma((n_aux - 1, n_orb - 1)),
            dma((n_aux - 1,)), dma((n_aux - 1,)),
            dma((3,)), dma((2,)),
        ],
        compiler_params=pltpu.CompilerParams(collective_id=0, has_side_effects=True, vmem_limit_bytes=67043328),
    )(ints, c_cat, c_rows, pick, weights)


def gram(t, mine, coul, n_aux):
    n_k, n_c, n_i, n_r, n_p = t.shape
    n_m, n_n = n_c * n_r, n_k * n_c * n_r
    n_col = n_n // n_aux

    def kernel(t_hbm, mine_hbm, coul_ref, g_ref, t_ref, mine_ref, acc, sq, side, k_send, k_got, c_send, c_got,
               load, load_m, ks_send, ks_recv, cs_send, cs_recv):
        j, k = lax.axis_index('aux'), lax.axis_index('orb')

        def load_t(i):
            return pltpu.make_async_copy(t_hbm.at[:, :, i], t_ref.at[i], load.at[i])

        def load_own(i):
            return pltpu.make_async_copy(mine_hbm.at[:, i], mine_ref.at[i], load_m.at[i])

        def k_copy(r):
            to = lax.rem(k + r, n_k)
            return pltpu.make_async_remote_copy(
                src_ref=k_send.at[to], dst_ref=k_got.at[r - 1], send_sem=ks_send.at[r - 1], recv_sem=ks_recv.at[r - 1],
                device_id={'orb': to}, device_id_type=MESH)

        def c_copy(r):
            to = lax.rem(j + n_aux - r, n_aux)
            return pltpu.make_async_remote_copy(
                src_ref=c_send.at[to], dst_ref=c_got.at[r - 1], send_sem=cs_send.at[r - 1], recv_sem=cs_recv.at[r - 1],
                device_id={'aux': to}, device_id_type=MESH)

        for i in range(n_i):
            load_t(i).start()
            load_own(i).start()
        barrier = pltpu.get_barrier_semaphore()
        for r in range(1, n_aux):
            pl.semaphore_signal(barrier, inc=1, device_id={'aux': lax.rem(j + r, n_aux)}, device_id_type=MESH)
        for r in range(1, n_k):
            pl.semaphore_signal(barrier, inc=1, device_id={'orb': lax.rem(k + r, n_k)}, device_id_type=MESH)
        acc[...] = jnp.zeros_like(acc)
        sq[...] = jnp.zeros_like(sq)
        nt = (((1,), (1,)), ((), ()))

        @pl.loop(0, n_i)
        def _(i):
            load_t(i).wait()
            load_own(i).wait()
            all_t = t_ref[i].reshape(n_n, n_p)
            own = mine_ref[i].reshape(n_m, n_p)
            _, mid, low = parts3(own)
            left = jnp.concatenate([all_t, mid, low], axis=0)
            acc[...] += lax.dot_general(left, all_t, nt, preferred_element_type=F32)
            sq[...] += lax.dot_general(mid, mid, nt, preferred_element_type=F32)

        put = lax.broadcasted_iota(jnp.int32, (n_m, n_n), 1) == lax.broadcasted_iota(jnp.int32, (n_m, n_n), 0) + k * n_m
        own_sq = jnp.dot(0.5 * sq[...], put.astype(F32), precision=PRECISE, preferred_element_type=F32)
        side[...] = jnp.zeros_like(side)
        side[pl.ds(pl.multiple_of(k * n_m, 8), n_m), :] = acc[n_n:n_n + n_m, :] + acc[n_n + n_m:, :] + own_sq
        k_send[...] = (acc[:n_n, :] + side[...] + side[...].T).reshape(n_k, n_m, n_n)
        pl.semaphore_wait(barrier, n_aux + n_k - 2)
        for r in range(1, n_k):
            k_copy(r).start()
        for r in range(1, n_k):
            k_copy(r).wait()
        total = k_send[k]
        for r in range(1, n_k):
            total += k_got[r - 1]
        for to in range(n_aux):
            c_send[to] = total[:, to * n_col:(to + 1) * n_col]
        for r in range(1, n_aux):
            c_copy(r).start()
        g_ref[j] = 2.0 * coul_ref[j] - c_send[j]
        for r in range(1, n_aux):
            c_copy(r).wait()
            d = lax.rem(j + r, n_aux)
            g_ref[d] = 2.0 * coul_ref[d] - c_got[r - 1]

    any_spec = pl.BlockSpec(memory_space=pl.ANY)
    vmem = pl.BlockSpec(memory_space=pltpu.VMEM)
    dma = pltpu.SemaphoreType.DMA
    return pl.pallas_call(
        kernel,
        out_shape=jax.ShapeDtypeStruct((n_aux, n_m, n_col), F32),
        in_specs=[any_spec, any_spec, vmem],
        out_specs=vmem,
        scratch_shapes=[
            pltpu.VMEM((n_i, n_k, n_c, n_r, n_p), BF16), pltpu.VMEM((n_i, n_c, n_r, n_p), F32),
            pltpu.VMEM((n_n + 2 * n_m, n_n), F32), pltpu.VMEM((n_m, n_m), F32), pltpu.VMEM((n_n, n_n), F32),
            pltpu.VMEM((n_k, n_m, n_n), F32), pltpu.VMEM((n_k - 1, n_m, n_n), F32),
            pltpu.VMEM((n_aux, n_m, n_col), F32), pltpu.VMEM((n_aux - 1, n_m, n_col), F32),
            dma((n_i,)), dma((n_i,)), dma((n_k - 1,)), dma((n_k - 1,)), dma((n_aux - 1,)), dma((n_aux - 1,)),
        ],
        compiler_params=pltpu.CompilerParams(collective_id=1, has_side_effects=True, vmem_limit_bytes=67043328),
    )(t, mine, coul)


def solution(mesh):
    n_aux, n_orb = mesh.shape['aux'], mesh.shape['orb']

    def local_fock(ints, metric, orbitals):
        n_q, n_m, n_l = ints.shape
        n_d, _, n_i = orbitals.shape
        n_p = n_aux * n_q
        n_c = n_m // (2 * SUB)
        pad_p = round_up(n_p, LANES)
        n_t = n_q // Q_TILE
        pad_q = n_t * LANES
        pad_di = round_up(n_d * n_i, LANES)
        k = lax.axis_index('orb')

        metric_pad = jnp.pad(metric.reshape(n_t, Q_TILE, n_p), ((0, 0), (0, LANES - Q_TILE), (0, pad_p - n_p))).reshape(pad_q, pad_p)
        m_hi, m_mid, m_low = split3(metric_pad)
        fit_w = jnp.concatenate([m_hi, m_mid, m_low, m_hi, m_mid, m_hi], axis=0)

        c_all = jnp.pad(orbitals.transpose(1, 0, 2).reshape(n_l, n_d * n_i), ((0, 0), (0, pad_di - n_d * n_i)))
        c_hi, c_mid, c_low = split3(c_all)
        c_cat = jnp.concatenate([c_hi, c_mid, c_low, c_hi, c_mid, c_hi], axis=0)
        c_rows = lax.dynamic_slice_in_dim(c_all, k * n_m, n_m, axis=0)
        lane = jnp.arange(pad_di)[None, :] // n_i
        pick = (lane == jnp.arange(2 * SUB)[:, None]).astype(F32)
        all_t, mine, coul = fit_exchange(ints.reshape(n_q, n_m // SUB, SUB, n_l), c_cat, c_rows.reshape(n_m // SUB, SUB, pad_di), pick, fit_w, n_aux, n_orb, n_i)
        all_t = all_t.reshape(n_orb, n_c, n_i // n_orb, 2 * SUB, pad_p)
        mine = mine.reshape(n_c, n_i // n_orb, 2 * SUB, pad_p)
        return gram(all_t, mine, coul, n_aux)

    return jax.shard_map(local_fock, mesh=mesh, in_specs=(P(('sys', 'aux'), 'orb', None), P(('sys', 'aux'), None), P('sys', None, None)), out_specs=P('sys', 'orb', 'aux'), check_vma=False)
```

```python
import jax
import jax.numpy as jnp
from jax import lax
from jax.experimental import pallas as pl
from jax.experimental.pallas import tpu as pltpu
from jax.sharding import PartitionSpec as P

PRECISE = lax.Precision.HIGHEST
F32 = jnp.float32
BF16 = jnp.bfloat16
MESH = pl.DeviceIdType.MESH
LANES = 128
WIDE = 256
SUB = 8
Q_TILE = 112


def round_up(n, to):
    return (n + to - 1) // to * to


def parts3(x):
    hi = x.astype(BF16)
    rest = x - hi.astype(F32)
    mid = rest.astype(BF16)
    return hi, mid, (rest - mid.astype(F32)).astype(BF16)


def split3(x):
    hi = lax.reduce_precision(x, 8, 7)
    mid = lax.reduce_precision(x - hi, 8, 7)
    return hi.astype(BF16), mid.astype(BF16), (x - hi - mid).astype(BF16)


def fock(ints, c_cat, c_rows, pick, parts, n_aux, n_orb, n_i):
    n_q, n_g, sub, n_l = ints.shape
    n_c = n_g // 2
    n_m = n_g * sub
    n_p = parts[0].shape[1]
    order = (0, 1, 2, 0, 1, 0)
    n_di = c_cat.shape[1]
    n_v = n_di // LANES
    n_d = n_aux
    pad_q = (n_q // Q_TILE) * LANES
    n_t = n_q // Q_TILE
    n_rows = n_i * 2 * sub
    half_rows = n_rows // 2
    share = half_rows // n_orb
    units = 2 * n_c
    slots = 4
    n_col = n_l // n_aux
    group = 2 * sub
    n_ii = share // group
    m_rows = pad_q // n_orb
    own_at = (n_aux - 1) * pad_q
    n_g_rows = pick.shape[0]

    def kernel(b_ref, c_ref, crow_ref, pick_ref, w_hi, w_mid, w_low, g_ref, t_ref, mine_ref,
               b_buf, w_ref, t_buf, temp, acc, send, part, got, fit, out, g_send, g_got, f_send, f_got, w_vec, w_smem, j_send, j_got, coul,
               y_send, y_recv, x_send, x_recv, gx_send, gx_recv, gy_send, gy_recv, my_send, my_recv, mx_send, mx_recv,
               jy_send, jy_recv, loc, keep, load, load_w, ks_send, ks_recv, cs_send, cs_recv,
               t_in, mine_in, prod, sq, side, k_send, k_got, c_send, c_got):
        j, k = lax.axis_index('aux'), lax.axis_index('orb')
        w_in = [pltpu.make_async_copy((w_hi, w_mid, w_low)[p], w_ref.at[pl.ds(own_at + n * pad_q, pad_q)], load_w.at[n])
                for n, p in enumerate(order)]

        def load_b(c):
            return pltpu.make_async_copy(b_ref.at[:, pl.ds(2 * c, 2)], b_buf, loc.at[0])

        load_b(0).start()
        for copy in w_in:
            copy.start()
        barrier = pltpu.get_barrier_semaphore()
        for r in range(1, n_aux):
            pl.semaphore_signal(barrier, inc=1, device_id={'aux': lax.rem(j + r, n_aux)}, device_id_type=MESH)
        for r in range(1, n_orb):
            pl.semaphore_signal(barrier, inc=1, device_id={'orb': lax.rem(k + r, n_orb)}, device_id_type=MESH)

        def cut(c, piece):
            if piece >= 2:
                return pl.ds(0, half_rows), pl.ds((piece - 2) * LANES, LANES)
            return pl.ds(piece * half_rows, half_rows), slice(None)

        def y_copy(c, r, piece):
            to = lax.rem(j + n_aux - r, n_aux)
            rows, lanes = cut(c, piece)
            return pltpu.make_async_remote_copy(
                src_ref=send.at[c % 2, to, rows, lanes], dst_ref=got.at[c, r - 1, rows, lanes], send_sem=y_send.at[c, r - 1, piece],
                recv_sem=y_recv.at[c, r - 1, piece], device_id={'aux': to}, device_id_type=MESH)

        def pieces(c, h):
            return tuple(range(2, 2 + n_t)) if c == 0 and h == 0 else (h,)

        def x_copy(u, r):
            to = lax.rem(k + r, n_orb)
            return pltpu.make_async_remote_copy(
                src_ref=out.at[u % slots, to], dst_ref=t_ref.at[k, u], send_sem=x_send.at[u, r - 1],
                recv_sem=x_recv.at[u, r - 1], device_id={'orb': to}, device_id_type=MESH)

        def my_copy(r):
            to = lax.rem(j + n_aux - r, n_aux)
            return pltpu.make_async_remote_copy(
                src_ref=w_hi.at[pl.ds(pl.multiple_of(k * m_rows, m_rows), m_rows)],
                dst_ref=w_ref.at[pl.ds(pl.multiple_of((r - 1) * pad_q + k * m_rows, m_rows), m_rows)],
                send_sem=my_send.at[r - 1], recv_sem=my_recv.at[r - 1], device_id={'aux': to}, device_id_type=MESH)

        def mx_copy(r, o):
            rows = w_ref.at[pl.ds(pl.multiple_of((r - 1) * pad_q + k * m_rows, m_rows), m_rows)]
            return pltpu.make_async_remote_copy(
                src_ref=rows, dst_ref=rows, send_sem=mx_send.at[r - 1, o - 1], recv_sem=mx_recv.at[r - 1, o - 1],
                device_id={'orb': lax.rem(k + o, n_orb)}, device_id_type=MESH)

        def jy_copy(r):
            to = lax.rem(j + n_aux - r, n_aux)
            return pltpu.make_async_remote_copy(
                src_ref=j_send.at[to], dst_ref=j_got.at[r - 1], send_sem=jy_send.at[r - 1], recv_sem=jy_recv.at[r - 1],
                device_id={'aux': to}, device_id_type=MESH)

        def gx_copy(r):
            return pltpu.make_async_remote_copy(
                src_ref=g_send, dst_ref=g_got.at[r - 1], send_sem=gx_send.at[r - 1], recv_sem=gx_recv.at[r - 1],
                device_id={'orb': lax.rem(k + r, n_orb)}, device_id_type=MESH)

        def gy_copy(r):
            return pltpu.make_async_remote_copy(
                src_ref=f_send, dst_ref=f_got.at[r - 1], send_sem=gy_send.at[r - 1], recv_sem=gy_recv.at[r - 1],
                device_id={'aux': lax.rem(j + r, n_aux)}, device_id_type=MESH)

        def keep_copies(u):
            return (pltpu.make_async_copy(fit, mine_ref.at[u], keep.at[0]),
                    pltpu.make_async_copy(out.at[u % slots, k], t_ref.at[k, u], keep.at[1]))

        acc[...] = jnp.zeros_like(acc)
        t_buf[:, Q_TILE * sub:, :] = jnp.zeros((n_v, (LANES - Q_TILE) * sub, LANES), F32)

        def transform(c):
            load_b(c).wait()
            if c >= 2:
                for r in range(1, n_aux):
                    for piece in pieces(c - 2, 0) + pieces(c - 2, 1):
                        y_copy(c - 2, r, piece).wait_send()

            def q_tile(t):
                lanes = pl.ds(pl.multiple_of(t * LANES, LANES), LANES)

                @pl.loop(0, 2)
                def _(h):
                    q_rows = pl.ds(pl.multiple_of(t * Q_TILE, Q_TILE), Q_TILE)
                    hi, mid, low = parts3(b_buf[q_rows, h, :, :].reshape(Q_TILE * sub, n_l))
                    left = jnp.concatenate([hi, hi, hi, mid, mid, low], axis=1)
                    res = jnp.dot(left, c_ref[...], preferred_element_type=F32)
                    for v in range(n_v):
                        t_buf[v, 0:Q_TILE * sub, :] = res[:, v * LANES:(v + 1) * LANES]
                    for v in range(n_v):
                        part_di = slice(v * LANES, (v + 1) * LANES)
                        c_row = crow_ref[2 * c + h, :, part_di]
                        live = min(LANES, n_d * n_i - v * LANES)
                        total = acc[t, :, part_di]
                        for m in range(sub):
                            row = t_buf[v, pl.ds(m, LANES, stride=sub), :]
                            total += row * c_row[m:m + 1, :]
                            temp[h, pl.ds(v * LANES * sub + m, live, stride=sub), :] = row.T[:live, :]
                        acc[t, :, part_di] = total

                for d in range(n_d):
                    rows = pl.ds(d * n_i * sub, n_i * sub)
                    both = jnp.concatenate([temp[h, rows, :].reshape(n_i, sub, LANES) for h in range(2)], axis=1)
                    send[c % 2, d, :, lanes] = both.reshape(n_rows, LANES).astype(BF16)
                rows = pl.ds(pl.multiple_of(j * (n_i * sub), n_i * sub), n_i * sub)
                both = jnp.concatenate([temp[h, rows, :].reshape(n_i, sub, LANES) for h in range(2)], axis=1)
                for p, piece in enumerate(parts3(both.reshape(n_rows, LANES))):
                    part[c % 2, :, pl.ds(pl.multiple_of(p * pad_q + t * LANES, LANES), LANES)] = piece

            if c == 0:
                for t in range(n_t):
                    q_tile(t)
                    for r in range(1, n_aux):
                        y_copy(c, r, 2 + t).start()
                    if t == 0:
                        for r in range(1, n_aux):
                            my_copy(r).wait_recv()
                            for o in range(1, n_orb):
                                mx_copy(r, o).start()
                for r in range(1, n_aux):
                    y_copy(c, r, 1).start()
            else:
                pl.loop(0, n_t)(q_tile)
                for piece in (0, 1):
                    for r in range(1, n_aux):
                        y_copy(c, r, piece).start()
            if c + 1 < n_c:
                load_b(c + 1).start()

        def fit_half(c, h):
            u = 2 * c + h
            for piece in pieces(c, h):
                for r in range(1, n_aux):
                    y_copy(c, r, piece).wait_recv()
            if u > 0:
                for copy in keep_copies(u - 1):
                    copy.wait()
            if u >= slots:
                for r in range(1, n_orb):
                    x_copy(u - slots, r).wait_send()

            def tile(start, width):
                rows = slice(h * half_rows, (h + 1) * half_rows)
                cols = pl.ds(start, width)
                hi, mid, low = [part[c % 2, rows, p * pad_q:(p + 1) * pad_q] for p in range(3)]
                left = jnp.concatenate([got[c, r, rows, :] for r in range(n_aux - 1)] + [hi, hi, hi, mid, mid, low], axis=1)
                res = jnp.dot(left, w_ref[:, cols], preferred_element_type=F32).reshape(n_orb, share, width)
                out[u % slots, :, :, cols] = res.astype(BF16)
                for b in range(n_orb):
                    @pl.when(k == b)
                    def _(b=b):
                        fit[:, cols] = res[b]

            @pl.loop(0, n_p // WIDE)
            def _(n):
                tile(pl.multiple_of(n * WIDE, WIDE), WIDE)
            if n_p % WIDE:
                tile(n_p // WIDE * WIDE, n_p % WIDE)

            for r in range(1, n_orb):
                x_copy(u, r).start()
            for copy in keep_copies(u):
                copy.start()

        nt = (((1,), (1,)), ((), ()))
        pl.semaphore_wait(barrier, n_aux + n_orb - 2)
        for r in range(1, n_aux):
            my_copy(r).start()
        transform(0)
        transform(1)
        for copy in w_in:
            copy.wait()
        for r in range(1, n_aux):
            for o in range(1, n_orb):
                mx_copy(r, o).wait_recv()
        fit_half(0, 0)
        fit_half(0, 1)
        transform(2)
        load_b(0).start()
        g_send[...] = lax.dot_general(pick_ref[...], acc[...].reshape(n_t * LANES, n_di), nt, precision=PRECISE, preferred_element_type=F32)
        for r in range(1, n_orb):
            gx_copy(r).start()
        fit_half(1, 0)
        for r in range(1, n_orb):
            gx_copy(r).wait()
        gamma = g_send[...]
        for r in range(1, n_orb):
            gamma += g_got[r - 1]
        hi, mid, low = parts3(gamma)
        left = jnp.concatenate([hi, hi, hi, mid, mid, low], axis=1)
        f_send[...] = jnp.dot(left, w_ref[own_at:, :], preferred_element_type=F32)
        for r in range(1, n_aux):
            gy_copy(r).start()
        fit_half(1, 1)
        for r in range(1, n_aux):
            gy_copy(r).wait()
        gamma_fit = f_send[...]
        for r in range(1, n_aux):
            gamma_fit += f_got[r - 1]
        hi, mid, low = parts3(gamma_fit)
        m_hi, m_mid, m_low = [w_ref[own_at + p * pad_q:own_at + (p + 1) * pad_q, :] for p in range(3)]
        by_hi = lax.dot_general(jnp.concatenate([hi, mid, low], axis=0), m_hi, nt, preferred_element_type=F32)
        by_mid = lax.dot_general(jnp.concatenate([hi, mid], axis=0), m_mid, nt, preferred_element_type=F32)
        by_low = lax.dot_general(hi, m_low, nt, preferred_element_type=F32)
        n = n_g_rows
        small = by_low + by_mid[n:] + by_hi[2 * n:]
        w_vec[...] = by_hi[:n] + ((by_hi[n:2 * n] + by_mid[:n]) + small)
        to_smem = pltpu.make_async_copy(w_vec, w_smem, loc.at[2])
        to_smem.start()
        to_smem.wait()
        for c in range(n_c):
            if c > 0:
                fit_half(2, c - 1)
            load_b(c).wait()
            for h in range(2):
                total = [jnp.zeros((sub, n_l), F32) for _ in range(n_d)]
                for t in range(n_t):
                    def some(s, total):
                        total = list(total)
                        for u in range(8):
                            q = s * 8 + u
                            block = b_buf[t * Q_TILE + q, h]
                            for d in range(n_d):
                                total[d] = total[d] + block * w_smem[d, t * LANES + q]
                        return tuple(total)
                    total = lax.fori_loop(0, Q_TILE // 8, some, tuple(total))
                for d in range(n_d):
                    for to in range(n_aux):
                        j_send[to, d, (2 * c + h) * sub:(2 * c + h + 1) * sub, :] = total[d][:, to * n_col:(to + 1) * n_col]
            if c + 1 < n_c:
                load_b(c + 1).start()
        for r in range(1, n_aux):
            jy_copy(r).start()
        for r in range(1, n_aux):
            jy_copy(r).wait()
        coul[...] = j_send[j]
        for r in range(1, n_aux):
            coul[...] += j_got[r - 1]

        def t_load(h, i):
            slot = lax.rem(i, 2)
            rows = pl.ds(pl.multiple_of(i * group, group), group)
            return [pltpu.make_async_copy(t_ref.at[:, 2 * c + h, rows], t_in.at[slot, :, c], load.at[slot, c]) for c in range(n_c)] + [
                pltpu.make_async_copy(mine_ref.at[2 * c + h, rows], mine_in.at[slot, c], load.at[slot, n_c + c]) for c in range(n_c)]

        prod[...] = jnp.zeros_like(prod)
        sq[...] = jnp.zeros_like(sq)
        for h in range(2):
            if h == 1:
                for copy in keep_copies(units - 1):
                    copy.wait()
            for c in range(n_c):
                for r in range(1, n_orb):
                    x_copy(2 * c + h, r).wait_recv()
            for i in range(2):
                for copy in t_load(h, i):
                    copy.start()

            @pl.loop(0, n_ii)
            def _(i):
                for copy in t_load(h, i):
                    copy.wait()
                slot = lax.rem(i, 2)
                all_t = t_in[slot].reshape(n_l, n_p)
                _, mid, low = parts3(mine_in[slot].reshape(n_m, n_p))
                left = jnp.concatenate([all_t, mid, low], axis=0)
                prod[...] += lax.dot_general(left, all_t, nt, preferred_element_type=F32)
                sq[...] += lax.dot_general(mid, mid, nt, preferred_element_type=F32)

                @pl.when(i + 2 < n_ii)
                def _():
                    for copy in t_load(h, i + 2):
                        copy.start()

        def k_copy(r):
            to = lax.rem(k + r, n_orb)
            return pltpu.make_async_remote_copy(
                src_ref=k_send.at[to], dst_ref=k_got.at[r - 1], send_sem=ks_send.at[r - 1], recv_sem=ks_recv.at[r - 1],
                device_id={'orb': to}, device_id_type=MESH)

        def c_copy(r):
            to = lax.rem(j + n_aux - r, n_aux)
            return pltpu.make_async_remote_copy(
                src_ref=c_send.at[to], dst_ref=c_got.at[r - 1], send_sem=cs_send.at[r - 1], recv_sem=cs_recv.at[r - 1],
                device_id={'aux': to}, device_id_type=MESH)

        put = lax.broadcasted_iota(jnp.int32, (n_m, n_l), 1) == lax.broadcasted_iota(jnp.int32, (n_m, n_l), 0) + k * n_m
        own_sq = jnp.dot(0.5 * sq[...], put.astype(F32), precision=PRECISE, preferred_element_type=F32)
        side[...] = jnp.zeros_like(side)
        side[pl.ds(pl.multiple_of(k * n_m, 8), n_m), :] = prod[n_l:n_l + n_m, :] + prod[n_l + n_m:, :] + own_sq
        k_send[...] = (prod[:n_l, :] + side[...] + side[...].T).reshape(n_orb, n_m, n_l)
        for r in range(1, n_orb):
            k_copy(r).start()
        for r in range(1, n_orb):
            k_copy(r).wait()
        total = k_send[k]
        for r in range(1, n_orb):
            total += k_got[r - 1]
        for to in range(n_aux):
            c_send[to] = total[:, to * n_col:(to + 1) * n_col]
        for r in range(1, n_aux):
            c_copy(r).start()
        g_ref[j] = 2.0 * coul[j] - c_send[j]
        for r in range(1, n_aux):
            c_copy(r).wait()
            d = lax.rem(j + r, n_aux)
            g_ref[d] = 2.0 * coul[d] - c_got[r - 1]

        for r in range(1, n_aux):
            my_copy(r).wait_send()
            for o in range(1, n_orb):
                mx_copy(r, o).wait_send()
            for c in range(n_c - 2, n_c):
                for piece in pieces(c, 0) + pieces(c, 1):
                    y_copy(c, r, piece).wait_send()
        for u in range(units):
            for r in range(1, n_orb):
                if u >= units - slots:
                    x_copy(u, r).wait_send()

    any_spec = pl.BlockSpec(memory_space=pl.ANY)
    vmem = pl.BlockSpec(memory_space=pltpu.VMEM)
    dma = pltpu.SemaphoreType.DMA
    return pl.pallas_call(
        kernel,
        out_shape=(jax.ShapeDtypeStruct((n_d, n_m, n_col), F32), jax.ShapeDtypeStruct((n_orb, units, share, n_p), BF16),
                   jax.ShapeDtypeStruct((units, share, n_p), F32)),
        in_specs=[any_spec, vmem, vmem, vmem, any_spec, any_spec, any_spec],
        out_specs=(vmem, any_spec, any_spec),
        scratch_shapes=[
            pltpu.VMEM((n_q, 2, sub, n_l), F32),
            pltpu.VMEM((own_at + len(order) * pad_q, n_p), BF16),
            pltpu.VMEM((n_v, LANES * sub, LANES), F32),
            pltpu.VMEM((2, n_d * n_i * sub, LANES), F32),
            pltpu.VMEM((n_t, LANES, n_di), F32),
            pltpu.VMEM((2, n_d, n_rows, pad_q), BF16),
            pltpu.VMEM((2, n_rows, 3 * pad_q), BF16),
            pltpu.VMEM((n_c, n_aux - 1, n_rows, pad_q), BF16),
            pltpu.VMEM((share, n_p), F32),
            pltpu.VMEM((slots, n_orb, share, n_p), BF16),
            pltpu.VMEM((n_g_rows, pad_q), F32), pltpu.VMEM((n_orb - 1, n_g_rows, pad_q), F32),
            pltpu.VMEM((n_g_rows, n_p), F32), pltpu.VMEM((n_aux - 1, n_g_rows, n_p), F32),
            pltpu.VMEM((n_g_rows, pad_q), F32), pltpu.SMEM((n_g_rows, pad_q), F32),
            pltpu.VMEM((n_aux, n_d, n_m, n_col), F32), pltpu.VMEM((n_aux - 1, n_d, n_m, n_col), F32), pltpu.VMEM((n_d, n_m, n_col), F32),
            dma((n_c, n_aux - 1, 2 + n_t)), dma((n_c, n_aux - 1, 2 + n_t)), dma((units, n_orb - 1)), dma((units, n_orb - 1)),
            dma((n_orb - 1,)), dma((n_orb - 1,)), dma((n_aux - 1,)), dma((n_aux - 1,)),
            dma((n_aux - 1,)), dma((n_aux - 1,)), dma((n_aux - 1, n_orb - 1)), dma((n_aux - 1, n_orb - 1)),
            dma((n_aux - 1,)), dma((n_aux - 1,)),
            dma((3,)), dma((2,)),
            dma((2, 2 * n_c)), dma((len(order),)), dma((n_orb - 1,)), dma((n_orb - 1,)), dma((n_aux - 1,)), dma((n_aux - 1,)),
            pltpu.VMEM((2, n_orb, n_c, group, n_p), BF16), pltpu.VMEM((2, n_c, group, n_p), F32),
            pltpu.VMEM((n_l + 2 * n_m, n_l), F32), pltpu.VMEM((n_m, n_m), F32), pltpu.VMEM((n_l, n_l), F32),
            pltpu.VMEM((n_orb, n_m, n_l), F32), pltpu.VMEM((n_orb - 1, n_m, n_l), F32),
            pltpu.VMEM((n_aux, n_m, n_col), F32), pltpu.VMEM((n_aux - 1, n_m, n_col), F32),
        ],
        compiler_params=pltpu.CompilerParams(collective_id=0, has_side_effects=True, vmem_limit_bytes=67043328),
    )(ints, c_cat, c_rows, pick, *parts)[0]


def solution(mesh):
    n_aux, n_orb = mesh.shape['aux'], mesh.shape['orb']

    def local_fock(ints, metric, orbitals):
        n_q, n_m, n_l = ints.shape
        n_d, _, n_i = orbitals.shape
        n_p = n_aux * n_q
        pad_p = round_up(n_p, LANES)
        n_t = n_q // Q_TILE
        pad_q = n_t * LANES
        pad_di = round_up(n_d * n_i, LANES)
        k = lax.axis_index('orb')

        metric_pad = jnp.pad(metric.reshape(n_t, Q_TILE, n_p), ((0, 0), (0, LANES - Q_TILE), (0, pad_p - n_p))).reshape(pad_q, pad_p)
        c_all = jnp.pad(orbitals.transpose(1, 0, 2).reshape(n_l, n_d * n_i), ((0, 0), (0, pad_di - n_d * n_i)))
        c_hi, c_mid, c_low = split3(c_all)
        c_cat = jnp.concatenate([c_hi, c_mid, c_low, c_hi, c_mid, c_hi], axis=0)
        c_rows = lax.dynamic_slice_in_dim(c_all, k * n_m, n_m, axis=0)
        lane = jnp.arange(pad_di)[None, :] // n_i
        pick = (lane == jnp.arange(2 * SUB)[:, None]).astype(F32)
        return fock(ints.reshape(n_q, n_m // SUB, SUB, n_l), c_cat, c_rows.reshape(n_m // SUB, SUB, pad_di), pick, split3(metric_pad),
                    n_aux, n_orb, n_i)

    return jax.shard_map(local_fock, mesh=mesh, in_specs=(P(('sys', 'aux'), 'orb', None), P(('sys', 'aux'), None), P('sys', None, None)), out_specs=P('sys', 'orb', 'aux'), check_vma=False)
```

```python
import jax
import jax.numpy as jnp
from jax import lax
from jax.experimental import pallas as pl
from jax.experimental.pallas import tpu as pltpu
from jax.sharding import PartitionSpec as P

PRECISE = lax.Precision.HIGHEST
F32 = jnp.float32
BF16 = jnp.bfloat16
MESH = pl.DeviceIdType.MESH
LANES = 128
WIDE = 256
SUB = 8
Q_TILE = 112


def round_up(n, to):
    return (n + to - 1) // to * to


def parts3(x):
    hi = x.astype(BF16)
    rest = x - hi.astype(F32)
    mid = rest.astype(BF16)
    return hi, mid, (rest - mid.astype(F32)).astype(BF16)


def split3(x):
    hi = lax.reduce_precision(x, 8, 7)
    mid = lax.reduce_precision(x - hi, 8, 7)
    return hi.astype(BF16), mid.astype(BF16), (x - hi - mid).astype(BF16)


def fock(ints, c_cat, c_rows, pick, parts, n_aux, n_orb, n_i):
    n_q, n_g, sub, n_l = ints.shape
    n_c = n_g // 2
    n_m = n_g * sub
    n_p = parts[0].shape[1]
    order = (0, 1, 2, 0, 1, 0)
    n_di = c_cat.shape[1]
    n_v = n_di // LANES
    n_d = n_aux
    pad_q = (n_q // Q_TILE) * LANES
    n_t = n_q // Q_TILE
    n_rows = n_i * 2 * sub
    half_rows = n_rows // 2
    share = half_rows // n_orb
    units = 2 * n_c
    slots = 4
    n_col = n_l // n_aux
    group = 2 * sub
    n_ii = share // group
    m_rows = pad_q // n_orb
    own_at = (n_aux - 1) * pad_q
    n_g_rows = pick.shape[0]

    def kernel(b_ref, c_ref, crow_ref, pick_ref, w_hi, w_mid, w_low, g_ref, t_ref, mine_ref,
               b_buf, w_ref, t_buf, temp, acc, send, part, got, fit, out, g_send, g_got, f_send, f_got, w_vec, w_smem, j_send, j_got, coul,
               y_send, y_recv, x_send, x_recv, gx_send, gx_recv, gy_send, gy_recv, my_send, my_recv, mx_send, mx_recv,
               jy_send, jy_recv, loc, keep, load, load_w, ks_send, ks_recv, cs_send, cs_recv,
               t_in, mine_in, prod, sq, side, k_send, k_got, c_send, c_got):
        j, k = lax.axis_index('aux'), lax.axis_index('orb')
        w_in = [pltpu.make_async_copy((w_hi, w_mid, w_low)[p], w_ref.at[pl.ds(own_at + n * pad_q, pad_q)], load_w.at[n])
                for n, p in enumerate(order)]

        def load_b(c):
            return pltpu.make_async_copy(b_ref.at[:, pl.ds(2 * c, 2)], b_buf, loc.at[0])

        load_b(0).start()
        for copy in w_in:
            copy.start()
        barrier = pltpu.get_barrier_semaphore()
        for r in range(1, n_aux):
            pl.semaphore_signal(barrier, inc=1, device_id={'aux': lax.rem(j + r, n_aux)}, device_id_type=MESH)
        for r in range(1, n_orb):
            pl.semaphore_signal(barrier, inc=1, device_id={'orb': lax.rem(k + r, n_orb)}, device_id_type=MESH)

        def cut(c, piece):
            if piece >= 2:
                return pl.ds(0, half_rows), pl.ds((piece - 2) * LANES, LANES)
            return pl.ds(piece * half_rows, half_rows), slice(None)

        def y_copy(c, r, piece):
            to = lax.rem(j + n_aux - r, n_aux)
            rows, lanes = cut(c, piece)
            return pltpu.make_async_remote_copy(
                src_ref=send.at[c % 2, to, rows, lanes], dst_ref=got.at[c, r - 1, rows, lanes], send_sem=y_send.at[c, r - 1, piece],
                recv_sem=y_recv.at[c, r - 1, piece], device_id={'aux': to}, device_id_type=MESH)

        def pieces(c, h):
            return tuple(range(2, 2 + n_t)) if c == 0 and h == 0 else (h,)

        def x_copy(u, r):
            to = lax.rem(k + r, n_orb)
            return pltpu.make_async_remote_copy(
                src_ref=out.at[u % slots, to], dst_ref=t_ref.at[k, u], send_sem=x_send.at[u, r - 1],
                recv_sem=x_recv.at[u, r - 1], device_id={'orb': to}, device_id_type=MESH)

        def my_copy(r):
            to = lax.rem(j + n_aux - r, n_aux)
            return pltpu.make_async_remote_copy(
                src_ref=w_hi.at[pl.ds(pl.multiple_of(k * m_rows, m_rows), m_rows)],
                dst_ref=w_ref.at[pl.ds(pl.multiple_of((r - 1) * pad_q + k * m_rows, m_rows), m_rows)],
                send_sem=my_send.at[r - 1], recv_sem=my_recv.at[r - 1], device_id={'aux': to}, device_id_type=MESH)

        def mx_copy(r, o):
            rows = w_ref.at[pl.ds(pl.multiple_of((r - 1) * pad_q + k * m_rows, m_rows), m_rows)]
            return pltpu.make_async_remote_copy(
                src_ref=rows, dst_ref=rows, send_sem=mx_send.at[r - 1, o - 1], recv_sem=mx_recv.at[r - 1, o - 1],
                device_id={'orb': lax.rem(k + o, n_orb)}, device_id_type=MESH)

        def jy_copy(r):
            to = lax.rem(j + n_aux - r, n_aux)
            return pltpu.make_async_remote_copy(
                src_ref=j_send.at[to], dst_ref=j_got.at[r - 1], send_sem=jy_send.at[r - 1], recv_sem=jy_recv.at[r - 1],
                device_id={'aux': to}, device_id_type=MESH)

        def gx_copy(r):
            return pltpu.make_async_remote_copy(
                src_ref=g_send, dst_ref=g_got.at[r - 1], send_sem=gx_send.at[r - 1], recv_sem=gx_recv.at[r - 1],
                device_id={'orb': lax.rem(k + r, n_orb)}, device_id_type=MESH)

        def gy_copy(r):
            return pltpu.make_async_remote_copy(
                src_ref=f_send, dst_ref=f_got.at[r - 1], send_sem=gy_send.at[r - 1], recv_sem=gy_recv.at[r - 1],
                device_id={'aux': lax.rem(j + r, n_aux)}, device_id_type=MESH)

        def keep_copies(u):
            return (pltpu.make_async_copy(fit, mine_ref.at[u], keep.at[0]),
                    pltpu.make_async_copy(out.at[u % slots, k], t_ref.at[k, u], keep.at[1]))

        acc[...] = jnp.zeros_like(acc)
        t_buf[:, Q_TILE * sub:, :] = jnp.zeros((n_v, (LANES - Q_TILE) * sub, LANES), F32)

        def transform(c):
            load_b(c).wait()
            if c >= 2:
                for r in range(1, n_aux):
                    for piece in pieces(c - 2, 0) + pieces(c - 2, 1):
                        y_copy(c - 2, r, piece).wait_send()

            def q_tile(t):
                lanes = pl.ds(pl.multiple_of(t * LANES, LANES), LANES)

                @pl.loop(0, 2)
                def _(h):
                    q_rows = pl.ds(pl.multiple_of(t * Q_TILE, Q_TILE), Q_TILE)
                    hi, mid, low = parts3(b_buf[q_rows, h, :, :].reshape(Q_TILE * sub, n_l))
                    left = jnp.concatenate([hi, hi, hi, mid, mid, low], axis=1)
                    res = jnp.dot(left, c_ref[...], preferred_element_type=F32)
                    for v in range(n_v):
                        t_buf[v, 0:Q_TILE * sub, :] = res[:, v * LANES:(v + 1) * LANES]
                    for v in range(n_v):
                        part_di = slice(v * LANES, (v + 1) * LANES)
                        c_row = crow_ref[2 * c + h, :, part_di]
                        live = min(LANES, n_d * n_i - v * LANES)
                        total = acc[t, :, part_di]
                        for m in range(sub):
                            row = t_buf[v, pl.ds(m, LANES, stride=sub), :]
                            total += row * c_row[m:m + 1, :]
                            temp[h, pl.ds(v * LANES * sub + m, live, stride=sub), :] = row.T[:live, :]
                        acc[t, :, part_di] = total

                for d in range(n_d):
                    rows = pl.ds(d * n_i * sub, n_i * sub)
                    both = jnp.concatenate([temp[h, rows, :].reshape(n_i, sub, LANES) for h in range(2)], axis=1)
                    send[c % 2, d, :, lanes] = both.reshape(n_rows, LANES).astype(BF16)
                rows = pl.ds(pl.multiple_of(j * (n_i * sub), n_i * sub), n_i * sub)
                both = jnp.concatenate([temp[h, rows, :].reshape(n_i, sub, LANES) for h in range(2)], axis=1)
                for p, piece in enumerate(parts3(both.reshape(n_rows, LANES))):
                    part[c % 2, :, pl.ds(pl.multiple_of(p * pad_q + t * LANES, LANES), LANES)] = piece

            if c == 0:
                for t in range(n_t):
                    q_tile(t)
                    for r in range(1, n_aux):
                        y_copy(c, r, 2 + t).start()
                    if t == 0:
                        for r in range(1, n_aux):
                            my_copy(r).wait_recv()
                            for o in range(1, n_orb):
                                mx_copy(r, o).start()
                for r in range(1, n_aux):
                    y_copy(c, r, 1).start()
            else:
                pl.loop(0, n_t)(q_tile)
                for piece in (0, 1):
                    for r in range(1, n_aux):
                        y_copy(c, r, piece).start()
            if c + 1 < n_c:
                load_b(c + 1).start()

        def fit_half(c, h):
            u = 2 * c + h
            for piece in pieces(c, h):
                for r in range(1, n_aux):
                    y_copy(c, r, piece).wait_recv()
            if u > 0:
                for copy in keep_copies(u - 1):
                    copy.wait()
            if u >= slots:
                for r in range(1, n_orb):
                    x_copy(u - slots, r).wait_send()

            def tile(start, width):
                rows = slice(h * half_rows, (h + 1) * half_rows)
                cols = pl.ds(start, width)
                hi, mid, low = [part[c % 2, rows, p * pad_q:(p + 1) * pad_q] for p in range(3)]
                left = jnp.concatenate([got[c, r, rows, :] for r in range(n_aux - 1)] + [hi, hi, hi, mid, mid, low], axis=1)
                res = jnp.dot(left, w_ref[:, cols], preferred_element_type=F32).reshape(n_orb, share, width)
                out[u % slots, :, :, cols] = res.astype(BF16)
                for b in range(n_orb):
                    @pl.when(k == b)
                    def _(b=b):
                        fit[:, cols] = res[b]

            @pl.loop(0, n_p // WIDE)
            def _(n):
                tile(pl.multiple_of(n * WIDE, WIDE), WIDE)
            if n_p % WIDE:
                tile(n_p // WIDE * WIDE, n_p % WIDE)

            for r in range(1, n_orb):
                x_copy(u, r).start()
            for copy in keep_copies(u):
                copy.start()

        nt = (((1,), (1,)), ((), ()))
        pl.semaphore_wait(barrier, n_aux + n_orb - 2)
        for r in range(1, n_aux):
            my_copy(r).start()
        transform(0)
        transform(1)
        for copy in w_in:
            copy.wait()
        for r in range(1, n_aux):
            for o in range(1, n_orb):
                mx_copy(r, o).wait_recv()
        fit_half(0, 0)
        fit_half(0, 1)
        transform(2)
        load_b(0).start()
        g_send[...] = lax.dot_general(pick_ref[...], acc[...].reshape(n_t * LANES, n_di), nt, precision=PRECISE, preferred_element_type=F32)
        for r in range(1, n_orb):
            gx_copy(r).start()
        fit_half(1, 0)
        for r in range(1, n_orb):
            gx_copy(r).wait()
        gamma = g_send[...]
        for r in range(1, n_orb):
            gamma += g_got[r - 1]
        hi, mid, low = parts3(gamma)
        left = jnp.concatenate([hi, hi, hi, mid, mid, low], axis=1)
        f_send[...] = jnp.dot(left, w_ref[own_at:, :], preferred_element_type=F32)
        for r in range(1, n_aux):
            gy_copy(r).start()
        fit_half(1, 1)
        for r in range(1, n_aux):
            gy_copy(r).wait()
        gamma_fit = f_send[...]
        for r in range(1, n_aux):
            gamma_fit += f_got[r - 1]
        hi, mid, low = parts3(gamma_fit)
        m_hi, m_mid, m_low = [w_ref[own_at + p * pad_q:own_at + (p + 1) * pad_q, :] for p in range(3)]
        by_hi = lax.dot_general(jnp.concatenate([hi, mid, low], axis=0), m_hi, nt, preferred_element_type=F32)
        by_mid = lax.dot_general(jnp.concatenate([hi, mid], axis=0), m_mid, nt, preferred_element_type=F32)
        by_low = lax.dot_general(hi, m_low, nt, preferred_element_type=F32)
        n = n_g_rows
        small = by_low + by_mid[n:] + by_hi[2 * n:]
        w_vec[...] = by_hi[:n] + ((by_hi[n:2 * n] + by_mid[:n]) + small)
        to_smem = pltpu.make_async_copy(w_vec, w_smem, loc.at[2])
        to_smem.start()
        to_smem.wait()
        for c in range(n_c):
            if c < 2:
                fit_half(2, c)
            load_b(c).wait()
            for h in range(2):
                total = [jnp.zeros((sub, n_l), F32) for _ in range(n_d)]
                for t in range(n_t):
                    def some(s, total):
                        total = list(total)
                        for u in range(8):
                            q = s * 8 + u
                            block = b_buf[t * Q_TILE + q, h]
                            for d in range(n_d):
                                total[d] = total[d] + block * w_smem[d, t * LANES + q]
                        return tuple(total)
                    total = lax.fori_loop(0, Q_TILE // 8, some, tuple(total))
                for d in range(n_d):
                    for to in range(n_aux):
                        j_send[to, d, (2 * c + h) * sub:(2 * c + h + 1) * sub, :] = total[d][:, to * n_col:(to + 1) * n_col]
            if c + 1 < n_c:
                load_b(c + 1).start()
        for r in range(1, n_aux):
            jy_copy(r).start()
        for r in range(1, n_aux):
            jy_copy(r).wait()
        coul[...] = j_send[j]
        for r in range(1, n_aux):
            coul[...] += j_got[r - 1]

        def t_load(h, i):
            slot = lax.rem(i, 2)
            rows = pl.ds(pl.multiple_of(i * group, group), group)
            return [pltpu.make_async_copy(t_ref.at[:, 2 * c + h, rows], t_in.at[slot, :, c], load.at[slot, c]) for c in range(n_c)] + [
                pltpu.make_async_copy(mine_ref.at[2 * c + h, rows], mine_in.at[slot, c], load.at[slot, n_c + c]) for c in range(n_c)]

        prod[...] = jnp.zeros_like(prod)
        sq[...] = jnp.zeros_like(sq)
        for h in range(2):
            if h == 1:
                for copy in keep_copies(units - 1):
                    copy.wait()
            for c in range(n_c):
                for r in range(1, n_orb):
                    x_copy(2 * c + h, r).wait_recv()
            for i in range(2):
                for copy in t_load(h, i):
                    copy.start()

            @pl.loop(0, n_ii)
            def _(i):
                for copy in t_load(h, i):
                    copy.wait()
                slot = lax.rem(i, 2)
                all_t = t_in[slot].reshape(n_l, n_p)
                _, mid, low = parts3(mine_in[slot].reshape(n_m, n_p))
                left = jnp.concatenate([all_t, mid, low], axis=0)
                prod[...] += lax.dot_general(left, all_t, nt, preferred_element_type=F32)
                sq[...] += lax.dot_general(mid, mid, nt, preferred_element_type=F32)

                @pl.when(i + 2 < n_ii)
                def _():
                    for copy in t_load(h, i + 2):
                        copy.start()

        def k_copy(r):
            to = lax.rem(k + r, n_orb)
            return pltpu.make_async_remote_copy(
                src_ref=k_send.at[to], dst_ref=k_got.at[r - 1], send_sem=ks_send.at[r - 1], recv_sem=ks_recv.at[r - 1],
                device_id={'orb': to}, device_id_type=MESH)

        def c_copy(r):
            to = lax.rem(j + n_aux - r, n_aux)
            return pltpu.make_async_remote_copy(
                src_ref=c_send.at[to], dst_ref=c_got.at[r - 1], send_sem=cs_send.at[r - 1], recv_sem=cs_recv.at[r - 1],
                device_id={'aux': to}, device_id_type=MESH)

        put = lax.broadcasted_iota(jnp.int32, (n_m, n_l), 1) == lax.broadcasted_iota(jnp.int32, (n_m, n_l), 0) + k * n_m
        own_sq = jnp.dot(0.5 * sq[...], put.astype(F32), precision=PRECISE, preferred_element_type=F32)
        side[...] = jnp.zeros_like(side)
        side[pl.ds(pl.multiple_of(k * n_m, 8), n_m), :] = prod[n_l:n_l + n_m, :] + prod[n_l + n_m:, :] + own_sq
        k_send[...] = (prod[:n_l, :] + side[...] + side[...].T).reshape(n_orb, n_m, n_l)
        for r in range(1, n_orb):
            k_copy(r).start()
        for r in range(1, n_orb):
            k_copy(r).wait()
        total = k_send[k]
        for r in range(1, n_orb):
            total += k_got[r - 1]
        for to in range(n_aux):
            c_send[to] = total[:, to * n_col:(to + 1) * n_col]
        for r in range(1, n_aux):
            c_copy(r).start()
        g_ref[j] = 2.0 * coul[j] - c_send[j]
        for r in range(1, n_aux):
            c_copy(r).wait()
            d = lax.rem(j + r, n_aux)
            g_ref[d] = 2.0 * coul[d] - c_got[r - 1]

        for r in range(1, n_aux):
            my_copy(r).wait_send()
            for o in range(1, n_orb):
                mx_copy(r, o).wait_send()
            for c in range(n_c - 2, n_c):
                for piece in pieces(c, 0) + pieces(c, 1):
                    y_copy(c, r, piece).wait_send()
        for u in range(units):
            for r in range(1, n_orb):
                if u >= units - slots:
                    x_copy(u, r).wait_send()

    any_spec = pl.BlockSpec(memory_space=pl.ANY)
    vmem = pl.BlockSpec(memory_space=pltpu.VMEM)
    dma = pltpu.SemaphoreType.DMA
    return pl.pallas_call(
        kernel,
        out_shape=(jax.ShapeDtypeStruct((n_d, n_m, n_col), F32), jax.ShapeDtypeStruct((n_orb, units, share, n_p), BF16),
                   jax.ShapeDtypeStruct((units, share, n_p), F32)),
        in_specs=[any_spec, vmem, vmem, vmem, any_spec, any_spec, any_spec],
        out_specs=(vmem, any_spec, any_spec),
        scratch_shapes=[
            pltpu.VMEM((n_q, 2, sub, n_l), F32),
            pltpu.VMEM((own_at + len(order) * pad_q, n_p), BF16),
            pltpu.VMEM((n_v, LANES * sub, LANES), F32),
            pltpu.VMEM((2, n_d * n_i * sub, LANES), F32),
            pltpu.VMEM((n_t, LANES, n_di), F32),
            pltpu.VMEM((2, n_d, n_rows, pad_q), BF16),
            pltpu.VMEM((2, n_rows, 3 * pad_q), BF16),
            pltpu.VMEM((n_c, n_aux - 1, n_rows, pad_q), BF16),
            pltpu.VMEM((share, n_p), F32),
            pltpu.VMEM((slots, n_orb, share, n_p), BF16),
            pltpu.VMEM((n_g_rows, pad_q), F32), pltpu.VMEM((n_orb - 1, n_g_rows, pad_q), F32),
            pltpu.VMEM((n_g_rows, n_p), F32), pltpu.VMEM((n_aux - 1, n_g_rows, n_p), F32),
            pltpu.VMEM((n_g_rows, pad_q), F32), pltpu.SMEM((n_g_rows, pad_q), F32),
            pltpu.VMEM((n_aux, n_d, n_m, n_col), F32), pltpu.VMEM((n_aux - 1, n_d, n_m, n_col), F32), pltpu.VMEM((n_d, n_m, n_col), F32),
            dma((n_c, n_aux - 1, 2 + n_t)), dma((n_c, n_aux - 1, 2 + n_t)), dma((units, n_orb - 1)), dma((units, n_orb - 1)),
            dma((n_orb - 1,)), dma((n_orb - 1,)), dma((n_aux - 1,)), dma((n_aux - 1,)),
            dma((n_aux - 1,)), dma((n_aux - 1,)), dma((n_aux - 1, n_orb - 1)), dma((n_aux - 1, n_orb - 1)),
            dma((n_aux - 1,)), dma((n_aux - 1,)),
            dma((3,)), dma((2,)),
            dma((2, 2 * n_c)), dma((len(order),)), dma((n_orb - 1,)), dma((n_orb - 1,)), dma((n_aux - 1,)), dma((n_aux - 1,)),
            pltpu.VMEM((2, n_orb, n_c, group, n_p), BF16), pltpu.VMEM((2, n_c, group, n_p), F32),
            pltpu.VMEM((n_l + 2 * n_m, n_l), F32), pltpu.VMEM((n_m, n_m), F32), pltpu.VMEM((n_l, n_l), F32),
            pltpu.VMEM((n_orb, n_m, n_l), F32), pltpu.VMEM((n_orb - 1, n_m, n_l), F32),
            pltpu.VMEM((n_aux, n_m, n_col), F32), pltpu.VMEM((n_aux - 1, n_m, n_col), F32),
        ],
        compiler_params=pltpu.CompilerParams(collective_id=0, has_side_effects=True, vmem_limit_bytes=67043328),
    )(ints, c_cat, c_rows, pick, *parts)[0]


def solution(mesh):
    n_aux, n_orb = mesh.shape['aux'], mesh.shape['orb']

    def local_fock(ints, metric, orbitals):
        n_q, n_m, n_l = ints.shape
        n_d, _, n_i = orbitals.shape
        n_p = n_aux * n_q
        pad_p = round_up(n_p, LANES)
        n_t = n_q // Q_TILE
        pad_q = n_t * LANES
        pad_di = round_up(n_d * n_i, LANES)
        k = lax.axis_index('orb')

        metric_pad = jnp.pad(metric.reshape(n_t, Q_TILE, n_p), ((0, 0), (0, LANES - Q_TILE), (0, pad_p - n_p))).reshape(pad_q, pad_p)
        c_all = jnp.pad(orbitals.transpose(1, 0, 2).reshape(n_l, n_d * n_i), ((0, 0), (0, pad_di - n_d * n_i)))
        c_hi, c_mid, c_low = split3(c_all)
        c_cat = jnp.concatenate([c_hi, c_mid, c_low, c_hi, c_mid, c_hi], axis=0)
        c_rows = lax.dynamic_slice_in_dim(c_all, k * n_m, n_m, axis=0)
        lane = jnp.arange(pad_di)[None, :] // n_i
        pick = (lane == jnp.arange(2 * SUB)[:, None]).astype(F32)
        return fock(ints.reshape(n_q, n_m // SUB, SUB, n_l), c_cat, c_rows.reshape(n_m // SUB, SUB, pad_di), pick, split3(metric_pad),
                    n_aux, n_orb, n_i)

    return jax.shard_map(local_fock, mesh=mesh, in_specs=(P(('sys', 'aux'), 'orb', None), P(('sys', 'aux'), None), P('sys', None, None)), out_specs=P('sys', 'orb', 'aux'), check_vma=False)
```
